128 devices in a mesh: dp: 32 (over y, z, core), mp: 4 (over x).
Axes of the slice: x: 4, y: 4, z: 4, core: 2. Of those that a mesh axis runs over, the one named last changes fastest.
Arguments:
- gradients: bfloat16 [4, 16, 1024, 1024], P(None, 'mp', 'dp'), as said below
- statistics: float32 [4, 32, 1024, 1024], P('mp', 'dp'), as said below
- accumulator: float32 [4, 16, 1024, 1024], P(None, 'mp', 'dp'), may hold values from 0.25 to 4
Outputs:
- update: float32 [4, 16, 1024, 1024], P(None, 'mp', 'dp')
- statistics_new: float32 [4, 32, 1024, 1024], P('mp', 'dp')
- accumulator_new: float32 [4, 16, 1024, 1024], P(None, 'mp', 'dp')
The draws below stay inside these ranges and needn't reach their ends.
Inputs may be any that keep to these rules, and one draw needn't show every extreme that they name: `gradients`: Real-valued gradient blocks. `statistics`: each 1024 x 1024 statistic is symmetric positive definite.
All inputs are finite; a program needn't handle non-finite values.
Results may differ from the reference program's by a relative error of at most 0.005.
The reference program's roundings to bfloat16 on the way count: a program that leaves them out, or rounds other values in their place, can miss the bound.
Values may be sent and summed in bfloat16 or wider, within the bound.
A program may use at most 64 MiB of HBM per device.

```python
import math
import jax
import jax.numpy as jnp
from jax import lax

B = 1024
ITERS = 3
RB = 4
CB = 16
CB_MP = 4
BLKS = 16
N_MP = 4


def draw_gradients(key, part):
    subkeys = jax.random.split(key, 3)
    gaussian = jax.random.normal(subkeys[0], (RB, CB, B, B), jnp.float32)
    row_scale = 10.0 ** jax.random.uniform(subkeys[1], (RB, CB, B, 1), jnp.float32)
    col_scale = 10.0 ** jax.random.uniform(subkeys[2], (RB, CB, 1, B), jnp.float32)
    rising = (3.0 ** (jnp.arange(B, dtype=jnp.float32) / B))[:, None]
    values = gaussian * row_scale * col_scale * rising
    return values.astype(jnp.bfloat16)


def draw_statistics(key, part):
    spread = 2.0

    def one_matrix(position):
        matrix_key = jax.random.fold_in(key, position)
        noise_key, scale_key = jax.random.split(matrix_key)
        gaussian = jax.random.normal(noise_key, (B, B), jnp.float32)
        wishart = jnp.dot(gaussian, gaussian.T, precision=lax.Precision.HIGHEST) / B + 0.5 * jnp.eye(B, dtype=jnp.float32)
        diagonal_scale = jnp.exp(jax.random.uniform(scale_key, (B,), jnp.float32) * jnp.log(spread))
        return 0.25 * diagonal_scale[:, None] * wishart * diagonal_scale[None, :]
    matrices = lax.map(one_matrix, jnp.arange(N_MP * 2 * BLKS, dtype=jnp.int32))
    return matrices.reshape(N_MP, 2 * BLKS, B, B)


def shard_levels(own_key, extent, cuts, smallest, high):
    def one(dim, blocks):
        heights = jax.random.uniform(jax.random.fold_in(jax.random.fold_in(own_key, 6), dim), (blocks,), jnp.float32, smallest / len(cuts), high / len(cuts))
        return jnp.repeat(jnp.exp(heights), extent[dim] // blocks).reshape((-1,) + (1,) * (len(extent) - dim - 1))

    factor_of = one(*cuts[0])
    for cut in cuts[1:]:
        factor_of = factor_of * one(*cut)
    return factor_of


def setup_inputs(seed: int = 0) -> dict:
    streams_of = jax.random.split(jax.random.key(seed), 4)
    gradients = draw_gradients(jax.random.fold_in(streams_of[3], 71), 0)
    statistics = draw_statistics(jax.random.fold_in(streams_of[3], 71), 0)
    accumulator = jnp.clip(jnp.exp(math.log(4.0) - 2.7725887 * jax.random.uniform(streams_of[2], (RB, CB, B, B), jnp.float32) ** shard_levels(streams_of[2], (RB, CB, B, B), ((1, 4), (2, 32)), -0.2, 0.2)), 0.25, 4.0)
    return {"gradients": gradients, "statistics": statistics, "accumulator": accumulator}


def matmul(left, right):
    return jnp.dot(left.astype(jnp.float32), right.astype(jnp.float32), precision=lax.Precision.HIGHEST)

def inverse_root(statistic):
    identity = jnp.eye(statistic.shape[0], dtype=jnp.float32)
    frob_norm = jnp.sqrt(jnp.sum(statistic * statistic) + 1e-06)
    newton_scale = 2.5 / frob_norm
    matrix = newton_scale * statistic
    root_iter = jnp.sqrt(jnp.sqrt(newton_scale)) * identity
    for iteration in range(ITERS):
        factor = (1.25 * identity - 0.25 * matrix).astype(jnp.bfloat16)
        root_iter = matmul(root_iter.astype(jnp.bfloat16), factor)
        if iteration + 1 < ITERS:
            square = matmul(factor, factor).astype(jnp.bfloat16)
            fourth = matmul(square, square).astype(jnp.bfloat16)
            matrix = matmul(fourth, matrix.astype(jnp.bfloat16))
    return root_iter

def reference(gradients, statistics, accumulator):
    grads_wide = gradients.astype(jnp.float32)
    grad_total = jnp.sum(grads_wide * grads_wide)
    clip_factor = jnp.minimum(1.0, jnp.sqrt(RB * CB * B * B / (grad_total + 1e-06)))

    def one_block(position):
        mp_shard = position // BLKS
        local_block = position % BLKS
        row_block = (local_block // CB_MP).astype(jnp.int32)
        col_block = (mp_shard * CB_MP + local_block % CB_MP).astype(jnp.int32)
        zero_index = jnp.zeros((), jnp.int32)
        grad_block = lax.dynamic_slice(gradients, (row_block, col_block, zero_index, zero_index), (1, 1, B, B))[0, 0]
        stat_pair = lax.dynamic_slice(statistics, (mp_shard.astype(jnp.int32), (2 * local_block).astype(jnp.int32), zero_index, zero_index), (1, 2, B, B))[0]
        left_stat = 0.9 * stat_pair[0] + 0.1 / B * clip_factor * clip_factor * matmul(grad_block, grad_block.T)
        right_stat = 0.9 * stat_pair[1] + 0.1 / B * clip_factor * clip_factor * matmul(grad_block.T, grad_block)
        left_root = inverse_root(left_stat).astype(jnp.bfloat16)
        right_root = inverse_root(right_stat).astype(jnp.bfloat16)
        left_applied = matmul(left_root, grad_block).astype(jnp.bfloat16)
        product = matmul(left_applied, right_root)
        return (jnp.stack([left_stat, right_stat]), product)
    stats_all, products = lax.map(one_block, jnp.arange(N_MP * BLKS, dtype=jnp.int32))
    statistics_new = stats_all.reshape(N_MP, 2 * BLKS, B, B)
    preconditioned = products.reshape(N_MP, RB, CB_MP, B, B).transpose(1, 0, 2, 3, 4).reshape(RB, CB, B, B)
    scaled = clip_factor * grads_wide
    accumulated = accumulator + scaled * scaled
    graft_step = scaled / jnp.sqrt(accumulated)
    graft_ratio = jnp.sqrt(jnp.sum(graft_step * graft_step) / (jnp.sum(preconditioned * preconditioned) + 1e-06))
    return (graft_ratio * preconditioned, statistics_new, accumulated)
```

```python
import functools

import jax
import jax.numpy as jnp
from jax import lax
from jax.experimental import pallas as pl
from jax.experimental.pallas import tpu as pltpu
from jax.sharding import Mesh
from jax.sharding import PartitionSpec as P

F32 = jnp.float32
BF16 = jnp.bfloat16
MESH = pl.DeviceIdType.MESH
VMEM = pl.BlockSpec(memory_space=pltpu.VMEM)
ANY = pl.BlockSpec(memory_space=pl.ANY)

B = 1024
TILE = 256
NT = B // TILE
ROWS = 32
CHIPS = 16
ENTRIES = 4 * 16 * 1024 * 1024


def ring_distance(offset):
    return sum(min(step, 4 - step) for step in offset)


PLANE = sorted(
    [(dy, dz) for dy in range(4) for dz in range(4) if (dy, dz) != (0, 0)],
    key=lambda offset: -ring_distance(offset),
)
COLUMN = [(dx, dc) for dx in range(4) for dc in range(2) if (dx, dc) != (0, 0)]


class Place:
    def __init__(self):
        self.y, self.z, self.c, self.x = (lax.axis_index(a) for a in ("y", "z", "c", "mp"))
        self.chip = self.y * 4 + self.z
        self.column = self.x * 2 + self.c
        self.partner = {"c": 1 - self.c}

    def plane(self, offset):
        return {"y": lax.rem(self.y + offset[0], 4), "z": lax.rem(self.z + offset[1], 4)}

    def plane_chip(self, offset):
        return lax.rem(self.y + offset[0], 4) * 4 + lax.rem(self.z + offset[1], 4)

    def plane_source(self, offset):
        return lax.rem(self.y + 4 - offset[0], 4) * 4 + lax.rem(self.z + 4 - offset[1], 4)

    def in_column(self, offset):
        return {"mp": lax.rem(self.x + offset[0], 4), "c": lax.rem(self.c + offset[1], 2)}

    def greet(self):
        barrier = pltpu.get_barrier_semaphore()
        for offset in PLANE:
            pl.semaphore_signal(barrier, 1, device_id=self.plane(offset), device_id_type=MESH)
        for offset in COLUMN:
            pl.semaphore_signal(barrier, 1, device_id=self.in_column(offset), device_id_type=MESH)

    def met(self):
        pl.semaphore_wait(pltpu.get_barrier_semaphore(), len(PLANE) + len(COLUMN))


def remote(src, dst, send, recv, device):
    return pltpu.make_async_remote_copy(
        src_ref=src, dst_ref=dst, send_sem=send, recv_sem=recv, device_id=device, device_id_type=MESH
    )


def started(copies):
    for copy in copies:
        copy.start()
    return copies


def to_tile(value):
    value = value.reshape(-1, 8, value.shape[-1]).sum(0)
    return sum(value[:, k * 128 : (k + 1) * 128] for k in range(value.shape[1] // 128))


def plane_sends(place, tile, slots, sems):
    return started(
        [
            remote(tile, slots.at[place.chip], sems.at[0, i], sems.at[1, i], place.plane(offset))
            for i, offset in enumerate(PLANE)
        ]
    )


def column_sends(place, tile, slots, sems):
    return started(
        [
            remote(tile, slots.at[place.column], sems.at[0, i], sems.at[1, i], place.in_column(offset))
            for i, offset in enumerate(COLUMN)
        ]
    )


def gathered(copies, tile, slots, own):
    slots[own] = tile[...]
    for copy in copies:
        copy.wait()
    return functools.reduce(jnp.add, [slots[k] for k in range(slots.shape[0])])


def gather_kernel(
    grads, accum, whole, clip_out, accum_new, graft_out,
    own, accum_in, tile1, slots1, tile2, slots2,
    load_sem, bulk_sem, pass_sem, plane_sem, column_sem,
):
    place = Place()
    load_grads = pltpu.make_async_copy(grads, own, load_sem.at[0])
    load_accum = pltpu.make_async_copy(accum, accum_in, load_sem.at[1])
    load_grads.start()
    load_accum.start()
    place.greet()
    load_grads.wait()
    squares = jnp.zeros((8, B), F32)
    for block in range(CHIPS):
        wide = own[block].astype(F32)
        squares += (wide * wide).reshape(-1, 8, B).sum(0)
    tile1[...] = to_tile(squares)
    place.met()
    plane = plane_sends(place, tile1, slots1, plane_sem)
    bulk = started(
        [
            remote(
                own.at[place.plane_chip(offset)], whole.at[place.chip, place.c],
                bulk_sem.at[0, i], bulk_sem.at[1, i], place.plane(offset),
            )
            for i, offset in enumerate(PLANE)
        ]
    )
    passed = started(
        [
            remote(
                own.at[place.chip], whole.at[place.chip, place.c],
                pass_sem.at[0, 15], pass_sem.at[1, 15], place.partner,
            )
        ]
    )
    whole[place.chip, place.c] = own[place.chip]
    tile2[...] = gathered(plane, tile1, slots1, place.chip)
    column = column_sends(place, tile2, slots2, column_sem)
    load_accum.wait()
    total = jnp.sum(gathered(column, tile2, slots2, place.column), axis=(0, 1), keepdims=True)
    clip = jnp.minimum(1.0, jnp.sqrt(ENTRIES / (total + 1e-06)))
    clip_out[...] = jnp.broadcast_to(clip, (8, 128))
    graft = jnp.zeros((8, B), F32)
    for i in range(CHIPS):
        if i < 15:
            bulk[14 - i].wait_recv()
            source = place.plane_source(PLANE[14 - i])
            passed += started(
                [
                    remote(
                        whole.at[source, place.c], whole.at[source, place.c],
                        pass_sem.at[0, i], pass_sem.at[1, i], place.partner,
                    )
                ]
            )
        scaled = clip * own[i].astype(F32)
        square = scaled * scaled
        accumulated = accum_in[i] + square
        accum_new[i] = accumulated
        graft += (square / accumulated).reshape(-1, 8, B).sum(0)
    graft_out[...] = to_tile(graft)
    for copy in bulk:
        copy.wait_send()
    for copy in passed:
        copy.wait()


def gather(grads, accum):
    return pl.pallas_call(
        gather_kernel,
        name="gather",
        out_shape=(
            jax.ShapeDtypeStruct((CHIPS, 2, ROWS, B), BF16),
            jax.ShapeDtypeStruct((8, 128), F32),
            jax.ShapeDtypeStruct((CHIPS, ROWS, B), F32),
            jax.ShapeDtypeStruct((8, 128), F32),
        ),
        in_specs=[ANY, ANY],
        out_specs=(VMEM, VMEM, VMEM, VMEM),
        scratch_shapes=[
            pltpu.VMEM((CHIPS, ROWS, B), BF16),
            pltpu.VMEM((CHIPS, ROWS, B), F32),
            pltpu.VMEM((8, 128), F32),
            pltpu.VMEM((CHIPS, 8, 128), F32),
            pltpu.VMEM((8, 128), F32),
            pltpu.VMEM((8, 8, 128), F32),
            pltpu.SemaphoreType.DMA((2,)),
            pltpu.SemaphoreType.DMA((2, 15)),
            pltpu.SemaphoreType.DMA((2, 16)),
            pltpu.SemaphoreType.DMA((2, 15)),
            pltpu.SemaphoreType.DMA((2, 7)),
        ],
        compiler_params=pltpu.CompilerParams(collective_id=0, has_side_effects=True),
    )(grads, accum)


def dot(left, right, contract_left, contract_right):
    return lax.dot_general(
        left, right, (((contract_left,), (contract_right,)), ((), ())), preferred_element_type=F32
    )


def panels():
    for j in range(NT):
        yield slice(j * TILE, (j + 1) * TILE), slice(j * TILE, B), slice((j + 1) * TILE, B)


def symmetric_product(left, right, store):
    for rows, upper, lower in panels():
        value = dot(left[rows, :], right[:, upper], 1, 0)
        store(rows, upper, lower, value)


def mirrored_store(out):
    def store(rows, upper, lower, value):
        value = value.astype(BF16)
        out[rows, upper] = value
        if lower.start < B:
            out[lower, rows] = value[:, TILE:].T

    return store


def plus_diagonal(value, scale):
    row = lax.broadcasted_iota(jnp.int32, value.shape, 0)
    col = lax.broadcasted_iota(jnp.int32, value.shape, 1)
    return jnp.where(row == col, 1.25, 0.0) - scale * value


def factor_store(factor_out, matrix_out):
    def store(rows, upper, lower, value):
        factor = plus_diagonal(value, 0.25).astype(BF16)
        factor_out[rows, upper] = factor
        if lower.start < B:
            factor_out[lower, rows] = factor[:, TILE:].T
        if matrix_out is not None:
            matrix = value.astype(BF16)
            matrix_out[rows, upper] = matrix
            if lower.start < B:
                matrix_out[lower, rows] = matrix[:, TILE:].T

    return store


def roots_kernel(
    whole, clip_in, statistic, accum_in, statistic_new, root, accum_new,
    new, old, factor, matrix, root_a, root_b, square, fourth, sems,
):
    core = lax.axis_index("c")
    load = pltpu.make_async_copy(statistic, old, sems.at[0])
    load.start()
    put_accum = pltpu.make_async_copy(accum_in, accum_new, sems.at[1])
    put_accum.start()

    @pl.when(core == 0)
    def _():
        for rows, upper, _ in panels():
            new[rows, upper] = dot(whole[rows, :], whole[upper, :], 1, 1)

    @pl.when(core == 1)
    def _():
        for rows, upper, _ in panels():
            new[rows, upper] = dot(whole[:, rows], whole[:, upper], 0, 0)

    clip = clip_in[0:1, 0:1]
    weight = 0.1 / B * clip * clip
    load.wait()
    frob = jnp.zeros((8, 128), F32)
    for rows, upper, lower in panels():
        gram = new[rows, upper] * weight
        value = 0.9 * old[rows, upper] + gram
        new[rows, upper] = value
        frob += to_tile(value * value)
        if lower.start < B:
            value = 0.9 * old[lower, rows] + gram[:, TILE:].T
            new[lower, rows] = value
            frob += to_tile(value * value)
    put_new = pltpu.make_async_copy(new, statistic_new, sems.at[2])
    put_new.start()
    total = jnp.sum(to_tile(frob), axis=(0, 1), keepdims=True)
    scale = 2.5 / jnp.sqrt(total + 1e-06)
    start = jnp.sqrt(jnp.sqrt(scale)).astype(BF16).astype(F32)

    @pl.loop(0, B // ROWS)
    def _(i):
        rows = pl.ds(pl.multiple_of(i * ROWS, ROWS), ROWS)
        value = scale * new[rows, :]
        matrix[rows, :] = value.astype(BF16)
        row = lax.broadcasted_iota(jnp.int32, value.shape, 0) + i * ROWS
        col = lax.broadcasted_iota(jnp.int32, value.shape, 1)
        step = (jnp.where(row == col, 1.25, 0.0) - 0.25 * value).astype(BF16)
        factor[rows, :] = step
        root_a[rows, :] = (start * step.astype(F32)).astype(BF16)

    symmetric_product(factor, factor, mirrored_store(square))
    symmetric_product(square, square, mirrored_store(fourth))
    symmetric_product(fourth, matrix, factor_store(factor, square))
    symmetric_product(root_a, factor, mirrored_store(root_b))
    symmetric_product(factor, factor, mirrored_store(matrix))
    symmetric_product(matrix, matrix, mirrored_store(fourth))
    symmetric_product(fourth, square, factor_store(factor, None))
    symmetric_product(root_b, factor, mirrored_store(root))
    put_accum.wait()
    put_new.wait()


def roots(whole, clip, statistic, accum):
    return pl.pallas_call(
        roots_kernel,
        name="roots",
        out_shape=(
            jax.ShapeDtypeStruct((B, B), F32),
            jax.ShapeDtypeStruct((B, B), BF16),
            jax.ShapeDtypeStruct((CHIPS, ROWS, B), F32),
        ),
        in_specs=[VMEM, VMEM, ANY, VMEM],
        out_specs=(ANY, VMEM, ANY),
        scratch_shapes=[pltpu.VMEM((B, B), F32)] * 2
        + [pltpu.VMEM((B, B), BF16)] * 6
        + [pltpu.SemaphoreType.DMA((3,))],
        compiler_params=pltpu.CompilerParams(),
    )(whole, clip, statistic, accum)


RETURN = [PLANE[:8], PLANE[8:] + [(0, 0)]]


def apply_kernel(
    root, whole, graft, back, ratio_out,
    left_rows, right, applied, product, tile1, slots1, tile2, slots2,
    swap_sem, bulk_sem, plane_sem, column_sem,
):
    place = Place()
    place.greet()
    place.met()

    def apply_rows(rows_of, right_root):
        grads = whole[...].reshape(B, B)
        for offsets in RETURN:
            rows = jnp.concatenate([rows_of(place.plane_chip(o)) for o in offsets], axis=0)
            value = dot(rows, grads, 1, 0).astype(BF16)
            for k, o in enumerate(offsets):
                applied[place.plane_chip(o)] = value[k * ROWS : (k + 1) * ROWS]
        return right_root

    def multiply(right_root):
        squares = jnp.zeros((8, B), F32)
        for step, offsets in enumerate(RETURN):
            rows = jnp.concatenate([applied[place.plane_chip(o)] for o in offsets], axis=0)
            value = dot(rows, right_root[...].reshape(B, B), 1, 0)
            squares += (value * value).reshape(-1, 8, B).sum(0)
            if step == 1:
                tile1[0:8] = to_tile(squares)
                tile1[8:16] = graft[...]
                plane_sends(place, tile1, slots1, plane_sem)
            value = value.astype(BF16)
            for k, o in enumerate(offsets):
                chip = place.plane_chip(o)
                product[chip] = value[k * ROWS : (k + 1) * ROWS]
                if o != (0, 0):
                    i = PLANE.index(o)
                    remote(
                        product.at[chip], back.at[place.chip],
                        bulk_sem.at[0, i], bulk_sem.at[1, i], place.plane(o),
                    ).start()
                else:
                    back[place.chip] = value[k * ROWS : (k + 1) * ROWS]

    send_left = remote(root.at[:, 1], left_rows, swap_sem.at[0, 0], swap_sem.at[1, 0], place.partner)
    send_right = remote(root, right, swap_sem.at[0, 1], swap_sem.at[1, 1], place.partner)

    @pl.when(place.c == 0)
    def _():
        send_left.start()
        apply_rows(lambda chip: root[chip, 0], right)
        send_right.wait_recv()
        multiply(right)
        send_left.wait_send()

    @pl.when(place.c == 1)
    def _():
        send_right.start()
        send_left.wait_recv()
        apply_rows(lambda chip: left_rows[chip], root)
        multiply(root)
        send_right.wait_send()

    plane = [
        remote(tile1, slots1.at[place.chip], plane_sem.at[0, i], plane_sem.at[1, i], place.plane(o))
        for i, o in enumerate(PLANE)
    ]
    tile2[...] = gathered(plane, tile1, slots1, place.chip)
    column = column_sends(place, tile2, slots2, column_sem)
    total = gathered(column, tile2, slots2, place.column)
    update_total = jnp.sum(total[0:8], axis=(0, 1), keepdims=True)
    graft_total = jnp.sum(total[8:16], axis=(0, 1), keepdims=True)
    ratio_out[...] = jnp.broadcast_to(jnp.sqrt(graft_total / (update_total + 1e-06)), (8, 128))
    for i, o in enumerate(PLANE):
        remote(
            product.at[place.plane_chip(o)], back.at[place.chip],
            bulk_sem.at[0, i], bulk_sem.at[1, i], place.plane(o),
        ).wait()


def apply(root, whole, graft):
    return pl.pallas_call(
        apply_kernel,
        name="apply",
        out_shape=(
            jax.ShapeDtypeStruct((CHIPS, ROWS, B), BF16),
            jax.ShapeDtypeStruct((8, 128), F32),
        ),
        in_specs=[VMEM, VMEM, VMEM],
        out_specs=(VMEM, VMEM),
        scratch_shapes=[
            pltpu.VMEM((CHIPS, ROWS, B), BF16),
            pltpu.VMEM((CHIPS, 2, ROWS, B), BF16),
            pltpu.VMEM((CHIPS, ROWS, B), BF16),
            pltpu.VMEM((CHIPS, ROWS, B), BF16),
            pltpu.VMEM((16, 128), F32),
            pltpu.VMEM((CHIPS, 16, 128), F32),
            pltpu.VMEM((16, 128), F32),
            pltpu.VMEM((8, 16, 128), F32),
            pltpu.SemaphoreType.DMA((2, 2)),
            pltpu.SemaphoreType.DMA((2, 15)),
            pltpu.SemaphoreType.DMA((2, 15)),
            pltpu.SemaphoreType.DMA((2, 7)),
        ],
        compiler_params=pltpu.CompilerParams(collective_id=1, has_side_effects=True),
    )(root, whole, graft)


def on_device(gradients, statistics, accumulator):
    grads = gradients.reshape(CHIPS, ROWS, B)
    whole, clip, accum, graft = gather(grads, accumulator.reshape(CHIPS, ROWS, B))
    statistic_new, root, accum_new = roots(
        whole.reshape(B, B), clip, statistics.reshape(B, B), accum
    )
    back, ratio = apply(root.reshape(CHIPS, 2, ROWS, B), whole, graft)
    update = ratio[0, 0] * back.astype(F32)
    return (
        update.reshape(gradients.shape),
        statistic_new.reshape(statistics.shape),
        accum_new.reshape(accumulator.shape),
    )


def solution(mesh):
    finer = Mesh(mesh.devices.reshape(4, 4, 2, mesh.shape["mp"]), ("y", "z", "c", "mp"))
    dp = ("y", "z", "c")
    specs = (P(None, "mp", dp, None), P("mp", dp, None, None), P(None, "mp", dp, None))
    return jax.shard_map(on_device, mesh=finer, in_specs=specs, out_specs=specs, check_vma=False)
```

```python
import functools

import jax
import jax.numpy as jnp
from jax import lax
from jax.experimental import pallas as pl
from jax.experimental.pallas import tpu as pltpu
from jax.sharding import Mesh
from jax.sharding import PartitionSpec as P

F32 = jnp.float32
BF16 = jnp.bfloat16
MESH = pl.DeviceIdType.MESH
VMEM = pl.BlockSpec(memory_space=pltpu.VMEM)
HBM = pl.BlockSpec(memory_space=pltpu.MemorySpace.HBM)

B = 1024
TILE = 256
NT = B // TILE
ROWS = 32
CHIPS = 16
ENTRIES = 4 * 16 * 1024 * 1024


def ring_distance(offset):
    return sum(min(step, 4 - step) for step in offset)


PLANE = sorted(
    [(dy, dz) for dy in range(4) for dz in range(4) if (dy, dz) != (0, 0)],
    key=lambda offset: -ring_distance(offset),
)
COLUMN = [(dx, dc) for dx in range(4) for dc in range(2) if (dx, dc) != (0, 0)]


class Place:
    def __init__(self):
        self.y, self.z, self.c, self.x = (lax.axis_index(a) for a in ("y", "z", "c", "mp"))
        self.chip = self.y * 4 + self.z
        self.column = self.x * 2 + self.c
        self.partner = {"c": 1 - self.c}

    def plane(self, offset):
        return {"y": lax.rem(self.y + offset[0], 4), "z": lax.rem(self.z + offset[1], 4)}

    def plane_chip(self, offset):
        return lax.rem(self.y + offset[0], 4) * 4 + lax.rem(self.z + offset[1], 4)

    def plane_source(self, offset):
        return lax.rem(self.y + 4 - offset[0], 4) * 4 + lax.rem(self.z + 4 - offset[1], 4)

    def in_column(self, offset):
        return {"mp": lax.rem(self.x + offset[0], 4), "c": lax.rem(self.c + offset[1], 2)}

    def greet(self):
        barrier = pltpu.get_barrier_semaphore()
        for offset in PLANE:
            pl.semaphore_signal(barrier, 1, device_id=self.plane(offset), device_id_type=MESH)
        for offset in COLUMN:
            pl.semaphore_signal(barrier, 1, device_id=self.in_column(offset), device_id_type=MESH)

    def met(self):
        pl.semaphore_wait(pltpu.get_barrier_semaphore(), len(PLANE) + len(COLUMN))


def remote(src, dst, send, recv, device):
    return pltpu.make_async_remote_copy(
        src_ref=src, dst_ref=dst, send_sem=send, recv_sem=recv, device_id=device, device_id_type=MESH
    )


def started(copies):
    for copy in copies:
        copy.start()
    return copies


def to_tile(value):
    value = value.reshape(-1, 8, value.shape[-1]).sum(0)
    return sum(value[:, k * 128 : (k + 1) * 128] for k in range(value.shape[1] // 128))


def plane_sends(place, tile, slots, sems):
    return started(
        [
            remote(tile, slots.at[place.chip], sems.at[0, i], sems.at[1, i], place.plane(offset))
            for i, offset in enumerate(PLANE)
        ]
    )


def column_sends(place, tile, slots, sems):
    return started(
        [
            remote(tile, slots.at[place.column], sems.at[0, i], sems.at[1, i], place.in_column(offset))
            for i, offset in enumerate(COLUMN)
        ]
    )


def gathered(copies, tile, slots, own):
    slots[own] = tile[...]
    for copy in copies:
        copy.wait()
    return functools.reduce(jnp.add, [slots[k] for k in range(slots.shape[0])])


def gather_kernel(
    grads, accum, statistic, whole, clip_out, accum_new, graft_out, statistic_out,
    own, accum_in, tile1, slots1, tile2, slots2,
    load_sem, bulk_sem, pass_sem, plane_sem, column_sem,
):
    place = Place()
    load_grads = pltpu.make_async_copy(grads, own, load_sem.at[0])
    load_accum = pltpu.make_async_copy(accum, accum_in, load_sem.at[1])
    load_grads.start()
    load_statistic = pltpu.make_async_copy(statistic, statistic_out, load_sem.at[2])
    load_accum.start()
    load_statistic.start()
    place.greet()
    load_grads.wait()
    squares = jnp.zeros((8, B), F32)
    for block in range(CHIPS):
        wide = own[block].astype(F32)
        squares += (wide * wide).reshape(-1, 8, B).sum(0)
    tile1[...] = to_tile(squares)
    place.met()
    plane = plane_sends(place, tile1, slots1, plane_sem)
    bulk = started(
        [
            remote(
                own.at[place.plane_chip(offset)], whole.at[place.chip, place.c],
                bulk_sem.at[0, i], bulk_sem.at[1, i], place.plane(offset),
            )
            for i, offset in enumerate(PLANE)
        ]
    )
    passed = started(
        [
            remote(
                own.at[place.chip], whole.at[place.chip, place.c],
                pass_sem.at[0, 15], pass_sem.at[1, 15], place.partner,
            )
        ]
    )
    whole[place.chip, place.c] = own[place.chip]
    tile2[...] = gathered(plane, tile1, slots1, place.chip)
    column = column_sends(place, tile2, slots2, column_sem)
    load_accum.wait()
    total = jnp.sum(gathered(column, tile2, slots2, place.column), axis=(0, 1), keepdims=True)
    clip = jnp.minimum(1.0, jnp.sqrt(ENTRIES / (total + 1e-06)))
    clip_out[...] = jnp.broadcast_to(clip, (8, 128))
    graft = jnp.zeros((8, B), F32)
    for i in range(CHIPS):
        if i < 15:
            bulk[14 - i].wait_recv()
            source = place.plane_source(PLANE[14 - i])
            passed += started(
                [
                    remote(
                        whole.at[source, place.c], whole.at[source, place.c],
                        pass_sem.at[0, i], pass_sem.at[1, i], place.partner,
                    )
                ]
            )
        scaled = clip * own[i].astype(F32)
        square = scaled * scaled
        accumulated = accum_in[i] + square
        accum_new[i] = accumulated
        graft += (square / accumulated).reshape(-1, 8, B).sum(0)
    graft_out[...] = to_tile(graft)
    load_statistic.wait()
    for copy in bulk:
        copy.wait_send()
    for copy in passed:
        copy.wait()


def gather(grads, accum, statistic):
    return pl.pallas_call(
        gather_kernel,
        name="gather",
        out_shape=(
            jax.ShapeDtypeStruct((CHIPS, 2, ROWS, B), BF16),
            jax.ShapeDtypeStruct((8, 128), F32),
            jax.ShapeDtypeStruct((CHIPS, ROWS, B), F32),
            jax.ShapeDtypeStruct((8, 128), F32),
            jax.ShapeDtypeStruct((B, B), F32),
        ),
        in_specs=[HBM, HBM, HBM],
        out_specs=(VMEM, VMEM, VMEM, VMEM, VMEM),
        scratch_shapes=[
            pltpu.VMEM((CHIPS, ROWS, B), BF16),
            pltpu.VMEM((CHIPS, ROWS, B), F32),
            pltpu.VMEM((8, 128), F32),
            pltpu.VMEM((CHIPS, 8, 128), F32),
            pltpu.VMEM((8, 128), F32),
            pltpu.VMEM((8, 8, 128), F32),
            pltpu.SemaphoreType.DMA((3,)),
            pltpu.SemaphoreType.DMA((2, 15)),
            pltpu.SemaphoreType.DMA((2, 16)),
            pltpu.SemaphoreType.DMA((2, 15)),
            pltpu.SemaphoreType.DMA((2, 7)),
        ],
        compiler_params=pltpu.CompilerParams(collective_id=0, has_side_effects=True, vmem_limit_bytes=24 << 20),
    )(grads, accum, statistic)


def dot(left, right, contract_left, contract_right):
    return lax.dot_general(
        left, right, (((contract_left,), (contract_right,)), ((), ())), preferred_element_type=F32
    )


def panels():
    for j in range(NT):
        yield slice(j * TILE, (j + 1) * TILE), slice(j * TILE, B), slice((j + 1) * TILE, B)


def symmetric_product(left, right, store):
    for rows, upper, lower in panels():
        value = dot(left[rows, :], right[:, upper], 1, 0)
        store(rows, upper, lower, value)


def mirrored_store(out):
    def store(rows, upper, lower, value):
        value = value.astype(BF16)
        out[rows, upper] = value
        if lower.start < B:
            out[lower, rows] = value[:, TILE:].T

    return store


def plus_diagonal(value, scale):
    row = lax.broadcasted_iota(jnp.int32, value.shape, 0)
    col = lax.broadcasted_iota(jnp.int32, value.shape, 1)
    return jnp.where(row == col, 1.25, 0.0) - scale * value


def factor_store(factor_out, matrix_out):
    def store(rows, upper, lower, value):
        factor = plus_diagonal(value, 0.25).astype(BF16)
        factor_out[rows, upper] = factor
        if lower.start < B:
            factor_out[lower, rows] = factor[:, TILE:].T
        if matrix_out is not None:
            matrix = value.astype(BF16)
            matrix_out[rows, upper] = matrix
            if lower.start < B:
                matrix_out[lower, rows] = matrix[:, TILE:].T

    return store


def roots_kernel(
    whole, clip_in, old, accum_in, statistic_new, root, factor, accum_new,
    new, matrix, root_a, square, fourth, sems,
):
    core = lax.axis_index("c")
    put_accum = pltpu.make_async_copy(accum_in, accum_new, sems.at[0])
    put_accum.start()

    @pl.when(core == 0)
    def _():
        for rows, upper, _ in panels():
            new[rows, upper] = dot(whole[rows, :], whole[upper, :], 1, 1)

    @pl.when(core == 1)
    def _():
        for rows, upper, _ in panels():
            new[rows, upper] = dot(whole[:, rows], whole[:, upper], 0, 0)

    clip = clip_in[0:1, 0:1]
    weight = 0.1 / B * clip * clip
    frob = jnp.zeros((8, 128), F32)
    for rows, upper, lower in panels():
        gram = new[rows, upper] * weight
        value = 0.9 * old[rows, upper] + gram
        new[rows, upper] = value
        frob += to_tile(value * value)
        if lower.start < B:
            value = 0.9 * old[lower, rows] + gram[:, TILE:].T
            new[lower, rows] = value
            frob += to_tile(value * value)
    put_new = pltpu.make_async_copy(new, statistic_new, sems.at[1])
    put_new.start()
    total = jnp.sum(frob, axis=(0, 1), keepdims=True)
    scale = 2.5 / jnp.sqrt(total + 1e-06)
    start = jnp.sqrt(jnp.sqrt(scale)).astype(BF16).astype(F32)

    @pl.loop(0, B // ROWS)
    def _(i):
        rows = pl.ds(pl.multiple_of(i * ROWS, ROWS), ROWS)
        value = scale * new[rows, :]
        matrix[rows, :] = value.astype(BF16)
        row = lax.broadcasted_iota(jnp.int32, value.shape, 0) + i * ROWS
        col = lax.broadcasted_iota(jnp.int32, value.shape, 1)
        step = (jnp.where(row == col, 1.25, 0.0) - 0.25 * value).astype(BF16)
        factor[rows, :] = step
        root_a[rows, :] = (start * step.astype(F32)).astype(BF16)

    symmetric_product(factor, factor, mirrored_store(square))
    symmetric_product(square, square, mirrored_store(fourth))
    symmetric_product(fourth, matrix, factor_store(factor, square))
    symmetric_product(root_a, factor, mirrored_store(root))
    symmetric_product(factor, factor, mirrored_store(matrix))
    symmetric_product(matrix, matrix, mirrored_store(fourth))
    symmetric_product(fourth, square, factor_store(factor, None))
    put_accum.wait()
    put_new.wait()


def roots(whole, clip, statistic, accum):
    return pl.pallas_call(
        roots_kernel,
        name="roots",
        out_shape=(
            jax.ShapeDtypeStruct((B, B), F32),
            jax.ShapeDtypeStruct((B, B), BF16),
            jax.ShapeDtypeStruct((B, B), BF16),
            jax.ShapeDtypeStruct((CHIPS, ROWS, B), F32),
        ),
        in_specs=[VMEM, VMEM, VMEM, VMEM],
        out_specs=(HBM, VMEM, VMEM, HBM),
        scratch_shapes=[pltpu.VMEM((B, B), F32)]
        + [pltpu.VMEM((B, B), BF16)] * 4
        + [pltpu.SemaphoreType.DMA((2,))],
        compiler_params=pltpu.CompilerParams(vmem_limit_bytes=32 << 20),
    )(whole, clip, statistic, accum)


def apply_kernel(
    root, factor, whole, graft, back, ratio_out,
    both, applied, product, tile1, slots1, tile2, slots2,
    left_sem, right_sem, bulk_sem, plane_sem, column_sem,
):
    place = Place()
    place.greet()

    def swap_left(j):
        chips = pl.ds(4 * j, 4)
        return remote(
            both.at[0, chips, 1], both.at[0, chips, 1],
            left_sem.at[0, j], left_sem.at[1, j], place.partner,
        )

    def swap_right(j):
        part = (1, pl.ds(4 * j, 4), slice(None), slice(None), pl.ds(j * TILE, B - j * TILE))
        return remote(
            both.at[part], both.at[part], right_sem.at[0, j], right_sem.at[1, j], place.partner
        )

    def give_back(j, i):
        return remote(
            product.at[j, place.plane_chip(PLANE[i])], back.at[j, place.chip],
            bulk_sem.at[0, j, i], bulk_sem.at[1, j, i], place.plane(PLANE[i]),
        )

    for j, (rows, upper, lower) in enumerate(panels()):
        value = dot(root[rows, :], factor[:, upper], 1, 0).astype(BF16)
        both[place.c, 4 * j : 4 * j + 4, :, :, upper] = value.reshape(4, 2, ROWS, -1)
        if lower.start < B:
            mirror = value[:, TILE:].T
            both[place.c, 4 * j + 4 : CHIPS, :, :, rows] = mirror.reshape(-1, 2, ROWS, TILE)
        if j == 0:
            place.met()

        @pl.when(place.c == 0)
        def _(j=j):
            swap_left(j).start()

        @pl.when(place.c == 1)
        def _(j=j):
            swap_right(j).start()

    @pl.when(place.c == 1)
    def _():
        for j in range(NT):
            swap_left(j).wait_recv()

    left_rows = both[0, :, place.c].reshape(B // 2, B)
    applied[...] = dot(left_rows, whole[...], 1, 0).astype(BF16)
    squares = jnp.zeros((8, 128), F32)
    for j, (rows, upper, _) in enumerate(panels()):

        @pl.when(place.c == 0)
        def _(j=j):
            swap_right(j).wait_recv()

        right_rows = both[1, 4 * j : 4 * j + 4, :, :, upper].reshape(TILE, -1)
        value = dot(applied[:, upper], right_rows, 1, 1)
        if j:
            value += dot(applied[:, : j * TILE], both[1, : 4 * j, :, :, rows].reshape(-1, TILE), 1, 0)
        squares += to_tile(value * value)
        product[j] = value.astype(BF16).reshape(CHIPS, ROWS, TILE)
        if j == NT - 1:
            tile1[0:8] = squares
            tile1[8:16] = graft[...]
            plane = plane_sends(place, tile1, slots1, plane_sem)
        for i in range(len(PLANE)):
            give_back(j, i).start()
        back[j, place.chip] = product[j, place.chip]

    tile2[...] = gathered(plane, tile1, slots1, place.chip)
    column = column_sends(place, tile2, slots2, column_sem)
    total = gathered(column, tile2, slots2, place.column)
    update_total = jnp.sum(total[0:8], axis=(0, 1), keepdims=True)
    graft_total = jnp.sum(total[8:16], axis=(0, 1), keepdims=True)
    ratio_out[...] = jnp.broadcast_to(jnp.sqrt(graft_total / (update_total + 1e-06)), (8, 128))

    @pl.when(place.c == 0)
    def _():
        for j in range(NT):
            swap_left(j).wait_send()

    @pl.when(place.c == 1)
    def _():
        for j in range(NT):
            swap_right(j).wait_send()

    for j in range(NT):
        for i in range(len(PLANE)):
            give_back(j, i).wait()


def apply(root, factor, whole, graft):
    return pl.pallas_call(
        apply_kernel,
        name="apply",
        out_shape=(
            jax.ShapeDtypeStruct((NT, CHIPS, ROWS, TILE), BF16),
            jax.ShapeDtypeStruct((8, 128), F32),
        ),
        in_specs=[VMEM, VMEM, VMEM, VMEM],
        out_specs=(VMEM, VMEM),
        scratch_shapes=[
            pltpu.VMEM((2, CHIPS, 2, ROWS, B), BF16),
            pltpu.VMEM((B // 2, B), BF16),
            pltpu.VMEM((NT, CHIPS, ROWS, TILE), BF16),
            pltpu.VMEM((16, 128), F32),
            pltpu.VMEM((CHIPS, 16, 128), F32),
            pltpu.VMEM((16, 128), F32),
            pltpu.VMEM((8, 16, 128), F32),
            pltpu.SemaphoreType.DMA((2, NT)),
            pltpu.SemaphoreType.DMA((2, NT)),
            pltpu.SemaphoreType.DMA((2, NT, 15)),
            pltpu.SemaphoreType.DMA((2, 15)),
            pltpu.SemaphoreType.DMA((2, 7)),
        ],
        compiler_params=pltpu.CompilerParams(
            collective_id=1, has_side_effects=True, vmem_limit_bytes=24 << 20
        ),
    )(root, factor, whole, graft)


def scale_kernel(back, ratio, update, wide, sems):
    factor = ratio[0:1, 0:1]
    puts = []
    for group in range(4):
        for chip in range(4 * group, 4 * group + 4):
            for j in range(NT):
                wide[chip, :, j * TILE : (j + 1) * TILE] = factor * back[j, chip].astype(F32)
        chips = pl.ds(4 * group, 4)
        puts += started([pltpu.make_async_copy(wide.at[chips], update.at[chips], sems.at[group])])
    for put in puts:
        put.wait()


def scale(back, ratio):
    return pl.pallas_call(
        scale_kernel,
        name="scale",
        out_shape=jax.ShapeDtypeStruct((CHIPS, ROWS, B), F32),
        in_specs=[VMEM, VMEM],
        out_specs=HBM,
        scratch_shapes=[pltpu.VMEM((CHIPS, ROWS, B), F32), pltpu.SemaphoreType.DMA((4,))],
        compiler_params=pltpu.CompilerParams(vmem_limit_bytes=16 << 20),
    )(back, ratio)


def on_device(gradients, statistics, accumulator):
    in_hbm = functools.partial(
        pltpu.with_memory_space_constraint, memory_space=pltpu.MemorySpace.HBM
    )
    grads = gradients.reshape(CHIPS, ROWS, B)
    whole, clip, accum, graft, statistic = gather(
        in_hbm(grads), in_hbm(accumulator.reshape(CHIPS, ROWS, B)), in_hbm(statistics.reshape(B, B))
    )
    whole = whole.reshape(B, B)
    statistic_new, root, factor, accum_new = roots(whole, clip, statistic, accum)
    update = scale(*apply(root, factor, whole, graft))
    return (
        update.reshape(gradients.shape),
        statistic_new.reshape(statistics.shape),
        accum_new.reshape(accumulator.shape),
    )


def solution(mesh):
    finer = Mesh(mesh.devices.reshape(4, 4, 2, mesh.shape["mp"]), ("y", "z", "c", "mp"))
    dp = ("y", "z", "c")
    specs = (P(None, "mp", dp, None), P("mp", dp, None, None), P(None, "mp", dp, None))
    return jax.shard_map(on_device, mesh=finer, in_specs=specs, out_specs=specs, check_vma=False)
```

```python
import functools

import jax
import jax.numpy as jnp
from jax import lax
from jax.experimental import pallas as pl
from jax.experimental.pallas import tpu as pltpu
from jax.sharding import Mesh
from jax.sharding import PartitionSpec as P

F32 = jnp.float32
BF16 = jnp.bfloat16
MESH = pl.DeviceIdType.MESH
VMEM = pl.BlockSpec(memory_space=pltpu.VMEM)
HBM = pl.BlockSpec(memory_space=pltpu.MemorySpace.HBM)

B = 1024
TILE = 256
NT = B // TILE
ROWS = 32
CHIPS = 16
ENTRIES = 4 * 16 * 1024 * 1024


def ring_distance(offset):
    return sum(min(step, 4 - step) for step in offset)


PLANE = sorted(
    [(dy, dz) for dy in range(4) for dz in range(4) if (dy, dz) != (0, 0)],
    key=ring_distance,
)
COLUMN = [(dx, dc) for dx in range(4) for dc in range(2) if (dx, dc) != (0, 0)]


class Place:
    def __init__(self):
        self.y, self.z, self.c, self.x = (lax.axis_index(a) for a in ("y", "z", "c", "mp"))
        self.chip = self.y * 4 + self.z
        self.column = self.x * 2 + self.c
        self.partner = {"c": 1 - self.c}

    def plane(self, offset):
        return {"y": lax.rem(self.y + offset[0], 4), "z": lax.rem(self.z + offset[1], 4)}

    def plane_chip(self, offset):
        return lax.rem(self.y + offset[0], 4) * 4 + lax.rem(self.z + offset[1], 4)

    def plane_source(self, offset):
        return lax.rem(self.y + 4 - offset[0], 4) * 4 + lax.rem(self.z + 4 - offset[1], 4)

    def in_column(self, offset):
        return {"mp": lax.rem(self.x + offset[0], 4), "c": lax.rem(self.c + offset[1], 2)}

    def greet(self):
        barrier = pltpu.get_barrier_semaphore()
        for offset in PLANE:
            pl.semaphore_signal(barrier, 1, device_id=self.plane(offset), device_id_type=MESH)
        for offset in COLUMN:
            pl.semaphore_signal(barrier, 1, device_id=self.in_column(offset), device_id_type=MESH)

    def met(self):
        pl.semaphore_wait(pltpu.get_barrier_semaphore(), len(PLANE) + len(COLUMN))


def remote(src, dst, send, recv, device):
    return pltpu.make_async_remote_copy(
        src_ref=src, dst_ref=dst, send_sem=send, recv_sem=recv, device_id=device, device_id_type=MESH
    )


def started(copies):
    for copy in copies:
        copy.start()
    return copies


def to_tile(value):
    value = value.reshape(-1, 8, value.shape[-1]).sum(0)
    return sum(value[:, k * 128 : (k + 1) * 128] for k in range(value.shape[1] // 128))


def plane_sends(place, tile, slots, sems):
    return [
        remote(tile, slots.at[place.chip], sems.at[0, i], sems.at[1, i], place.plane(offset))
        for i, offset in enumerate(PLANE)
    ]


def column_sends(place, tile, slots, sems):
    return [
        remote(tile, slots.at[place.column], sems.at[0, i], sems.at[1, i], place.in_column(offset))
        for i, offset in enumerate(COLUMN)
    ]


def gathered(copies, tile, slots, own):
    slots[own] = tile[...]
    for copy in copies:
        copy.wait()
    return functools.reduce(jnp.add, [slots[k] for k in range(slots.shape[0])])


def gather_kernel(
    grads, accum, statistic, whole, clip_out, accum_new, graft_out, statistic_out,
    own, accum_in, tile1, slots1, tile2, slots2,
    load_sem, bulk_sem, pass_sem, plane_sem, column_sem,
):
    place = Place()
    load_grads = pltpu.make_async_copy(grads, own, load_sem.at[0])
    load_accum = pltpu.make_async_copy(accum, accum_in, load_sem.at[1])
    load_grads.start()
    load_statistic = pltpu.make_async_copy(statistic, statistic_out, load_sem.at[2])
    place.greet()
    load_grads.wait()
    squares = jnp.zeros((8, B), F32)
    for block in range(CHIPS):
        wide = own[block].astype(F32)
        squares += (wide * wide).reshape(-1, 8, B).sum(0)
    tile1[...] = to_tile(squares)
    load_accum.start()
    load_statistic.start()
    place.met()
    plane = started(plane_sends(place, tile1, slots1, plane_sem))
    bulk = started(
        [
            remote(
                own.at[place.plane_chip(offset)], whole.at[place.chip, place.c],
                bulk_sem.at[0, i], bulk_sem.at[1, i], place.plane(offset),
            )
            for i, offset in enumerate(PLANE)
        ]
    )
    passed = started(
        [
            remote(
                own.at[place.chip], whole.at[place.chip, place.c],
                pass_sem.at[0, 15], pass_sem.at[1, 15], place.partner,
            )
        ]
    )
    whole[place.chip, place.c] = own[place.chip]
    tile2[...] = gathered(plane, tile1, slots1, place.chip)
    column = started(column_sends(place, tile2, slots2, column_sem))
    load_accum.wait()
    total = jnp.sum(gathered(column, tile2, slots2, place.column), axis=(0, 1), keepdims=True)
    clip = jnp.minimum(1.0, jnp.sqrt(ENTRIES / (total + 1e-06)))
    clip_out[...] = jnp.broadcast_to(clip, (8, 128))
    graft = jnp.zeros((8, B), F32)
    for i in range(CHIPS):
        if i < 15:
            bulk[i].wait_recv()
            source = place.plane_source(PLANE[i])
            passed += started(
                [
                    remote(
                        whole.at[source, place.c], whole.at[source, place.c],
                        pass_sem.at[0, i], pass_sem.at[1, i], place.partner,
                    )
                ]
            )
        scaled = clip * own[i].astype(F32)
        square = scaled * scaled
        accumulated = accum_in[i] + square
        accum_new[i] = accumulated
        graft += (square / accumulated).reshape(-1, 8, B).sum(0)
    graft_out[...] = to_tile(graft)
    load_statistic.wait()
    for copy in bulk:
        copy.wait_send()
    for copy in passed:
        copy.wait()


def gather(grads, accum, statistic):
    return pl.pallas_call(
        gather_kernel,
        name="gather",
        out_shape=(
            jax.ShapeDtypeStruct((CHIPS, 2, ROWS, B), BF16),
            jax.ShapeDtypeStruct((8, 128), F32),
            jax.ShapeDtypeStruct((CHIPS, ROWS, B), F32),
            jax.ShapeDtypeStruct((8, 128), F32),
            jax.ShapeDtypeStruct((B, B), F32),
        ),
        in_specs=[HBM, HBM, HBM],
        out_specs=(VMEM, VMEM, VMEM, VMEM, VMEM),
        scratch_shapes=[
            pltpu.VMEM((CHIPS, ROWS, B), BF16),
            pltpu.VMEM((CHIPS, ROWS, B), F32),
            pltpu.VMEM((8, 128), F32),
            pltpu.VMEM((CHIPS, 8, 128), F32),
            pltpu.VMEM((8, 128), F32),
            pltpu.VMEM((8, 8, 128), F32),
            pltpu.SemaphoreType.DMA((3,)),
            pltpu.SemaphoreType.DMA((2, 15)),
            pltpu.SemaphoreType.DMA((2, 16)),
            pltpu.SemaphoreType.DMA((2, 15)),
            pltpu.SemaphoreType.DMA((2, 7)),
        ],
        compiler_params=pltpu.CompilerParams(collective_id=0, has_side_effects=True, vmem_limit_bytes=24 << 20),
    )(grads, accum, statistic)


def dot(left, right, contract_left, contract_right):
    return lax.dot_general(
        left, right, (((contract_left,), (contract_right,)), ((), ())), preferred_element_type=F32
    )


def panels():
    for j in range(NT):
        yield slice(j * TILE, (j + 1) * TILE), slice(j * TILE, B), slice((j + 1) * TILE, B)


def symmetric_product(left, right, store):
    for rows, upper, lower in panels():
        value = dot(left[rows, :], right[:, upper], 1, 0)
        store(rows, upper, lower, value)


def mirrored_store(out):
    def store(rows, upper, lower, value):
        value = value.astype(BF16)
        out[rows, upper] = value
        if lower.start < B:
            out[lower, rows] = value[:, TILE:].T

    return store


def plus_diagonal(value, scale):
    row = lax.broadcasted_iota(jnp.int32, value.shape, 0)
    col = lax.broadcasted_iota(jnp.int32, value.shape, 1)
    return jnp.where(row == col, 1.25, 0.0) - scale * value


def factor_store(factor_out, matrix_out):
    def store(rows, upper, lower, value):
        factor = plus_diagonal(value, 0.25).astype(BF16)
        factor_out[rows, upper] = factor
        if lower.start < B:
            factor_out[lower, rows] = factor[:, TILE:].T
        if matrix_out is not None:
            matrix = value.astype(BF16)
            matrix_out[rows, upper] = matrix
            if lower.start < B:
                matrix_out[lower, rows] = matrix[:, TILE:].T

    return store


def roots_kernel(
    whole, clip_in, old, accum_in, statistic_new, root_a, factor, matrix_out, accum_new,
    new, matrix, square, fourth, sems,
):
    core = lax.axis_index("c")
    put_accum = pltpu.make_async_copy(accum_in, accum_new, sems.at[0])
    put_accum.start()

    @pl.when(core == 0)
    def _():
        for rows, upper, _ in panels():
            new[rows, upper] = dot(whole[rows, :], whole[upper, :], 1, 1)

    @pl.when(core == 1)
    def _():
        for rows, upper, _ in panels():
            new[rows, upper] = dot(whole[:, rows], whole[:, upper], 0, 0)

    clip = clip_in[0:1, 0:1]
    weight = 0.1 / B * clip * clip
    frob = jnp.zeros((8, 128), F32)
    for rows, upper, lower in panels():
        gram = new[rows, upper] * weight
        value = 0.9 * old[rows, upper] + gram
        new[rows, upper] = value
        frob += to_tile(value * value)
        if lower.start < B:
            value = 0.9 * old[lower, rows] + gram[:, TILE:].T
            new[lower, rows] = value
            frob += to_tile(value * value)
    put_new = pltpu.make_async_copy(new, statistic_new, sems.at[1])
    put_new.start()
    total = jnp.sum(frob, axis=(0, 1), keepdims=True)
    scale = 2.5 / jnp.sqrt(total + 1e-06)
    start = jnp.sqrt(jnp.sqrt(scale)).astype(BF16).astype(F32)

    @pl.loop(0, B // ROWS)
    def _(i):
        rows = pl.ds(pl.multiple_of(i * ROWS, ROWS), ROWS)
        value = scale * new[rows, :]
        matrix[rows, :] = value.astype(BF16)
        row = lax.broadcasted_iota(jnp.int32, value.shape, 0) + i * ROWS
        col = lax.broadcasted_iota(jnp.int32, value.shape, 1)
        step = (jnp.where(row == col, 1.25, 0.0) - 0.25 * value).astype(BF16)
        factor[rows, :] = step
        root_a[rows, :] = (start * step.astype(F32)).astype(BF16)

    symmetric_product(factor, factor, mirrored_store(square))
    symmetric_product(square, square, mirrored_store(fourth))
    symmetric_product(fourth, matrix, factor_store(factor, matrix_out))
    put_accum.wait()
    put_new.wait()


def roots(whole, clip, statistic, accum):
    return pl.pallas_call(
        roots_kernel,
        name="roots",
        out_shape=(
            jax.ShapeDtypeStruct((B, B), F32),
            jax.ShapeDtypeStruct((B, B), BF16),
            jax.ShapeDtypeStruct((B, B), BF16),
            jax.ShapeDtypeStruct((B, B), BF16),
            jax.ShapeDtypeStruct((CHIPS, ROWS, B), F32),
        ),
        in_specs=[VMEM, VMEM, VMEM, VMEM],
        out_specs=(HBM, VMEM, VMEM, VMEM, HBM),
        scratch_shapes=[pltpu.VMEM((B, B), F32)]
        + [pltpu.VMEM((B, B), BF16)] * 3
        + [pltpu.SemaphoreType.DMA((2,))],
        compiler_params=pltpu.CompilerParams(vmem_limit_bytes=32 << 20),
    )(whole, clip, statistic, accum)


def apply_kernel(
    root_a, factor_a, matrix, whole, graft, back, ratio_out,
    root, factor, square, fourth, both, applied, product, tile1, slots1, tile2, slots2,
    left_sem, right_sem, bulk_sem, plane_sem, column_sem,
):
    place = Place()
    place.greet()

    def swap_left(j):
        chips = pl.ds(4 * j, 4)
        return remote(
            both.at[0, chips, 1], both.at[0, chips, 1],
            left_sem.at[0, j], left_sem.at[1, j], place.partner,
        )

    def swap_right(j):
        part = (1, pl.ds(4 * j, 4), slice(None), slice(None), pl.ds(j * TILE, B - j * TILE))
        return remote(
            both.at[part], both.at[part], right_sem.at[0, j], right_sem.at[1, j], place.partner
        )

    def give_back(j, i):
        return remote(
            product.at[j, place.plane_chip(PLANE[i])], back.at[j, place.chip],
            bulk_sem.at[0, j, i], bulk_sem.at[1, j, i], place.plane(PLANE[i]),
        )

    symmetric_product(root_a, factor_a, mirrored_store(root))
    symmetric_product(factor_a, factor_a, mirrored_store(square))
    symmetric_product(square, square, mirrored_store(fourth))
    symmetric_product(fourth, matrix, factor_store(factor, None))
    place.met()
    for j, (rows, upper, lower) in enumerate(panels()):
        value = dot(root[rows, :], factor[:, upper], 1, 0).astype(BF16)
        both[place.c, 4 * j : 4 * j + 4, :, :, upper] = value.reshape(4, 2, ROWS, -1)
        if lower.start < B:
            mirror = value[:, TILE:].T
            both[place.c, 4 * j + 4 : CHIPS, :, :, rows] = mirror.reshape(-1, 2, ROWS, TILE)

        if j % 2:

            @pl.when(place.c == 0)
            def _(j=j):
                swap_left(j - 1).start()
                swap_left(j).start()

            @pl.when(place.c == 1)
            def _(j=j):
                swap_right(j - 1).start()
                swap_right(j).start()

    for half in range(2):

        @pl.when(place.c == 1)
        def _(half=half):
            for j in (2 * half, 2 * half + 1):
                swap_left(j).wait_recv()

        left_rows = both[0, 8 * half : 8 * half + 8, place.c].reshape(TILE, B)
        applied[half * TILE : (half + 1) * TILE] = dot(left_rows, whole[...], 1, 0).astype(BF16)
    squares = jnp.zeros((8, 128), F32)
    for j, (rows, upper, _) in enumerate(panels()):

        if j == 0:

            @pl.when(place.c == 0)
            def _():
                for i in range(NT):
                    swap_right(i).wait_recv()

        right_rows = both[1, 4 * j : 4 * j + 4, :, :, upper].reshape(TILE, -1)
        value = dot(applied[:, upper], right_rows, 1, 1)
        if j:
            value += dot(applied[:, : j * TILE], both[1, : 4 * j, :, :, rows].reshape(-1, TILE), 1, 0)
        squares += to_tile(value * value)
        product[j] = value.astype(BF16).reshape(CHIPS, ROWS, TILE)
        if j == NT - 1:
            tile1[0:8] = squares
            tile1[8:16] = graft[...]
            plane = started(plane_sends(place, tile1, slots1, plane_sem))
        for panel in {0: [0], NT - 1: range(1, NT)}.get(j, []):
            for i in range(len(PLANE)):
                give_back(panel, i).start()
        back[j, place.chip] = product[j, place.chip]

    tile2[...] = gathered(plane, tile1, slots1, place.chip)
    column = started(column_sends(place, tile2, slots2, column_sem))
    total = gathered(column, tile2, slots2, place.column)
    update_total = jnp.sum(total[0:8], axis=(0, 1), keepdims=True)
    graft_total = jnp.sum(total[8:16], axis=(0, 1), keepdims=True)
    ratio_out[...] = jnp.broadcast_to(jnp.sqrt(graft_total / (update_total + 1e-06)), (8, 128))

    @pl.when(place.c == 0)
    def _():
        for j in range(NT):
            swap_left(j).wait_send()

    @pl.when(place.c == 1)
    def _():
        for j in range(NT):
            swap_right(j).wait_send()

    for j in range(NT):
        for i in range(len(PLANE)):
            give_back(j, i).wait()


def apply(root, factor, matrix, whole, graft):
    return pl.pallas_call(
        apply_kernel,
        name="apply",
        out_shape=(
            jax.ShapeDtypeStruct((NT, CHIPS, ROWS, TILE), BF16),
            jax.ShapeDtypeStruct((8, 128), F32),
        ),
        in_specs=[VMEM, VMEM, VMEM, VMEM, VMEM],
        out_specs=(VMEM, VMEM),
        scratch_shapes=[pltpu.VMEM((B, B), BF16)] * 4
        + [
            pltpu.VMEM((2, CHIPS, 2, ROWS, B), BF16),
            pltpu.VMEM((B // 2, B), BF16),
            pltpu.VMEM((NT, CHIPS, ROWS, TILE), BF16),
            pltpu.VMEM((16, 128), F32),
            pltpu.VMEM((CHIPS, 16, 128), F32),
            pltpu.VMEM((16, 128), F32),
            pltpu.VMEM((8, 16, 128), F32),
            pltpu.SemaphoreType.DMA((2, NT)),
            pltpu.SemaphoreType.DMA((2, NT)),
            pltpu.SemaphoreType.DMA((2, NT, 15)),
            pltpu.SemaphoreType.DMA((2, 15)),
            pltpu.SemaphoreType.DMA((2, 7)),
        ],
        compiler_params=pltpu.CompilerParams(
            collective_id=1, has_side_effects=True, vmem_limit_bytes=32 << 20
        ),
    )(root, factor, matrix, whole, graft)


def scale_kernel(back, ratio, update, wide, sems):
    factor = ratio[0:1, 0:1]
    puts = []
    for group in range(4):
        for chip in range(4 * group, 4 * group + 4):
            for j in range(NT):
                wide[chip, :, j * TILE : (j + 1) * TILE] = factor * back[j, chip].astype(F32)
        chips = pl.ds(4 * group, 4)
        puts += started([pltpu.make_async_copy(wide.at[chips], update.at[chips], sems.at[group])])
    for put in puts:
        put.wait()


def scale(back, ratio):
    return pl.pallas_call(
        scale_kernel,
        name="scale",
        out_shape=jax.ShapeDtypeStruct((CHIPS, ROWS, B), F32),
        in_specs=[VMEM, VMEM],
        out_specs=HBM,
        scratch_shapes=[pltpu.VMEM((CHIPS, ROWS, B), F32), pltpu.SemaphoreType.DMA((4,))],
        compiler_params=pltpu.CompilerParams(vmem_limit_bytes=16 << 20),
    )(back, ratio)


def on_device(gradients, statistics, accumulator):
    in_hbm = functools.partial(
        pltpu.with_memory_space_constraint, memory_space=pltpu.MemorySpace.HBM
    )
    grads = gradients.reshape(CHIPS, ROWS, B)
    whole, clip, accum, graft, statistic = gather(
        in_hbm(grads), in_hbm(accumulator.reshape(CHIPS, ROWS, B)), in_hbm(statistics.reshape(B, B))
    )
    whole = whole.reshape(B, B)
    statistic_new, root, factor, matrix, accum_new = roots(whole, clip, statistic, accum)
    update = scale(*apply(root, factor, matrix, whole, graft))
    return (
        update.reshape(gradients.shape),
        statistic_new.reshape(statistics.shape),
        accum_new.reshape(accumulator.shape),
    )


def solution(mesh):
    finer = Mesh(mesh.devices.reshape(4, 4, 2, mesh.shape["mp"]), ("y", "z", "c", "mp"))
    dp = ("y", "z", "c")
    specs = (P(None, "mp", dp, None), P("mp", dp, None, None), P(None, "mp", dp, None))
    return jax.shard_map(on_device, mesh=finer, in_specs=specs, out_specs=specs, check_vma=False)
```

```python
import functools

import jax
import jax.numpy as jnp
from jax import lax
from jax.experimental import pallas as pl
from jax.experimental.pallas import tpu as pltpu
from jax.sharding import Mesh
from jax.sharding import PartitionSpec as P

F32 = jnp.float32
BF16 = jnp.bfloat16
MESH = pl.DeviceIdType.MESH
VMEM = pl.BlockSpec(memory_space=pltpu.VMEM)
HBM = pl.BlockSpec(memory_space=pltpu.MemorySpace.HBM)

B = 1024
TILE = 256
NT = B // TILE
ROWS = 32
CHIPS = 16
ENTRIES = 4 * 16 * 1024 * 1024


def ring_distance(offset):
    return sum(min(step, 4 - step) for step in offset)


PLANE = sorted(
    [(dy, dz) for dy in range(4) for dz in range(4) if (dy, dz) != (0, 0)],
    key=lambda offset: (offset[0] == 2, ring_distance(offset)),
)
COLUMN = [(dx, dc) for dx in range(4) for dc in range(2) if (dx, dc) != (0, 0)]

ORDER = (0, 1, 3, 2)
POSITION = [ORDER.index(step) for step in range(4)]
SEND = sorted(range(len(PLANE)), key=lambda i: ring_distance(PLANE[i]))
RETURN = sorted(range(len(PLANE)), key=lambda i: -ring_distance(PLANE[i]))
EARLY = sum(offset[0] != 2 for offset in PLANE)


class Place:
    def __init__(self):
        self.y, self.z, self.c, self.x = (lax.axis_index(a) for a in ("y", "z", "c", "mp"))
        self.chip = self.y * 4 + self.z
        self.column = self.x * 2 + self.c
        self.partner = {"c": 1 - self.c}

    def plane(self, offset):
        return {"y": lax.rem(self.y + offset[0], 4), "z": lax.rem(self.z + offset[1], 4)}

    def plane_chip(self, offset):
        return lax.rem(self.y + offset[0], 4) * 4 + lax.rem(self.z + offset[1], 4)

    def slot_to(self, offset):
        return POSITION[offset[0]] * 4 + lax.rem(self.z + offset[1], 4)

    def slot_from(self, offset):
        return POSITION[(4 - offset[0]) % 4] * 4 + lax.rem(self.z + 4 - offset[1], 4)

    def landing(self, offset):
        return POSITION[(4 - offset[0]) % 4] * 4 + self.z

    def in_column(self, offset):
        return {"mp": lax.rem(self.x + offset[0], 4), "c": lax.rem(self.c + offset[1], 2)}

    def greet(self):
        barrier = pltpu.get_barrier_semaphore()
        for offset in PLANE:
            pl.semaphore_signal(barrier, 1, device_id=self.plane(offset), device_id_type=MESH)
        for offset in COLUMN:
            pl.semaphore_signal(barrier, 1, device_id=self.in_column(offset), device_id_type=MESH)

    def met(self):
        pl.semaphore_wait(pltpu.get_barrier_semaphore(), len(PLANE) + len(COLUMN))


def statistic_tiles():
    y, c = lax.axis_index("y"), lax.axis_index("c")
    starts = [((1 - c) * lax.rem(y + ORDER[p], 4) + c * p) * TILE for p in range(NT)]
    windows = [pl.ds(pl.multiple_of(start, TILE), TILE) for start in starts]
    for p in range(NT):
        for q in range(NT):
            kept = (slice(p * TILE, (p + 1) * TILE), slice(q * TILE, (q + 1) * TILE))
            yield p * NT + q, kept, (windows[p], windows[q])


def remote(src, dst, send, recv, device):
    return pltpu.make_async_remote_copy(
        src_ref=src, dst_ref=dst, send_sem=send, recv_sem=recv, device_id=device, device_id_type=MESH
    )


def started(copies):
    for copy in copies:
        copy.start()
    return copies


def to_tile(value):
    value = value.reshape(-1, 8, value.shape[-1]).sum(0)
    return sum(value[:, k * 128 : (k + 1) * 128] for k in range(value.shape[1] // 128))


def plane_sends(place, tile, slots, sems):
    return [
        remote(tile, slots.at[place.chip], sems.at[0, i], sems.at[1, i], place.plane(offset))
        for i, offset in enumerate(PLANE)
    ]


def column_sends(place, tile, slots, sems):
    return [
        remote(tile, slots.at[place.column], sems.at[0, i], sems.at[1, i], place.in_column(offset))
        for i, offset in enumerate(COLUMN)
    ]


def gathered(copies, tile, slots, own):
    slots[own] = tile[...]
    for copy in copies:
        copy.wait()
    return functools.reduce(jnp.add, [slots[k] for k in range(slots.shape[0])])


def gather_kernel(
    grads, accum, statistic, whole, clip_out, accum_new, graft_out, statistic_out, gram,
    own, accum_in, tile1, slots1, tile2, slots2,
    load_sem, tile_sem, bulk_sem, pass_sem, plane_sem, column_sem,
):
    place = Place()
    load_grads = pltpu.make_async_copy(grads, own, load_sem.at[0])
    load_accum = pltpu.make_async_copy(accum, accum_in, load_sem.at[1])
    load_grads.start()
    place.greet()
    load_grads.wait()
    squares = jnp.zeros((8, B), F32)
    for block in range(CHIPS):
        wide = own[block].astype(F32)
        squares += (wide * wide).reshape(-1, 8, B).sum(0)
    tile1[...] = to_tile(squares)
    load_accum.start()
    load_tiles = started(
        [
            pltpu.make_async_copy(statistic.at[theirs], statistic_out.at[kept], tile_sem.at[i])
            for i, kept, theirs in statistic_tiles()
        ]
    )
    place.met()
    plane = started(plane_sends(place, tile1, slots1, plane_sem))
    bulk = [
        remote(
            own.at[place.plane_chip(offset)], whole.at[place.landing(offset), place.c],
            bulk_sem.at[0, i], bulk_sem.at[1, i], place.plane(offset),
        )
        for i, offset in enumerate(PLANE)
    ]
    started([bulk[i] for i in SEND])

    def pass_on(i):
        bulk[i].wait_recv()
        slot = place.slot_from(PLANE[i])
        return started(
            [
                remote(
                    whole.at[slot, place.c], whole.at[slot, place.c],
                    pass_sem.at[0, i], pass_sem.at[1, i], place.partner,
                )
            ]
        )

    passed = started(
        [
            remote(
                own.at[place.chip], whole.at[place.z, place.c],
                pass_sem.at[0, 15], pass_sem.at[1, 15], place.partner,
            )
        ]
    )
    whole[place.z, place.c] = own[place.chip]
    tile2[...] = gathered(plane, tile1, slots1, place.chip)
    column = started(column_sends(place, tile2, slots2, column_sem))
    load_accum.wait()
    total = jnp.sum(gathered(column, tile2, slots2, place.column), axis=(0, 1), keepdims=True)
    clip = jnp.minimum(1.0, jnp.sqrt(ENTRIES / (total + 1e-06)))
    clip_out[...] = jnp.broadcast_to(clip, (8, 128))
    graft = jnp.zeros((8, B), F32)
    for i in range(CHIPS):
        if i < EARLY:
            passed += pass_on(i)
        scaled = clip * own[i].astype(F32)
        square = scaled * scaled
        accumulated = accum_in[i] + square
        accum_new[i] = accumulated
        graft += (square / accumulated).reshape(-1, 8, B).sum(0)
    graft_out[...] = to_tile(graft)
    for i in range(EARLY, len(PLANE)):
        passed += pass_on(i)
    for copy in passed[: EARLY + 1]:
        copy.wait_recv()
    early_gram(place.c, whole, gram)
    for copy in load_tiles:
        copy.wait()
    for copy in bulk:
        copy.wait_send()
    for copy in passed[: EARLY + 1]:
        copy.wait_send()
    for copy in passed[EARLY + 1 :]:
        copy.wait()


def early_gram(core, whole, gram):
    known = (NT - 1) * TILE

    @pl.when(core == 0)
    def _():
        rows = whole[:12].reshape(known, B)
        for j in range(NT - 1):
            part = rows[j * TILE :]
            gram[j * TILE : (j + 1) * TILE, j * TILE : known] = dot(part[:TILE], part, 1, 1)

    @pl.when(core == 1)
    def _():
        for rows, upper, _ in panels():
            left = whole[:12, :, :, rows].reshape(known, TILE)
            gram[rows, upper] = dot(left, whole[:12, :, :, upper].reshape(known, -1), 0, 0)


def gather(grads, accum, statistic):
    return pl.pallas_call(
        gather_kernel,
        name="gather",
        out_shape=(
            jax.ShapeDtypeStruct((CHIPS, 2, ROWS, B), BF16),
            jax.ShapeDtypeStruct((8, 128), F32),
            jax.ShapeDtypeStruct((CHIPS, ROWS, B), F32),
            jax.ShapeDtypeStruct((8, 128), F32),
            jax.ShapeDtypeStruct((B, B), F32),
            jax.ShapeDtypeStruct((B, B), F32),
        ),
        in_specs=[HBM, HBM, HBM],
        out_specs=(VMEM, VMEM, VMEM, VMEM, VMEM, VMEM),
        scratch_shapes=[
            pltpu.VMEM((CHIPS, ROWS, B), BF16),
            pltpu.VMEM((CHIPS, ROWS, B), F32),
            pltpu.VMEM((8, 128), F32),
            pltpu.VMEM((CHIPS, 8, 128), F32),
            pltpu.VMEM((8, 128), F32),
            pltpu.VMEM((8, 8, 128), F32),
            pltpu.SemaphoreType.DMA((2,)),
            pltpu.SemaphoreType.DMA((NT * NT,)),
            pltpu.SemaphoreType.DMA((2, 15)),
            pltpu.SemaphoreType.DMA((2, 16)),
            pltpu.SemaphoreType.DMA((2, 15)),
            pltpu.SemaphoreType.DMA((2, 7)),
        ],
        compiler_params=pltpu.CompilerParams(collective_id=0, has_side_effects=True, vmem_limit_bytes=24 << 20),
    )(grads, accum, statistic)


def dot(left, right, contract_left, contract_right):
    return lax.dot_general(
        left, right, (((contract_left,), (contract_right,)), ((), ())), preferred_element_type=F32
    )


def panels():
    for j in range(NT):
        yield slice(j * TILE, (j + 1) * TILE), slice(j * TILE, B), slice((j + 1) * TILE, B)


def symmetric_product(left, right, store):
    for rows, upper, lower in panels():
        value = dot(left[rows, :], right[:, upper], 1, 0)
        store(rows, upper, lower, value)


def mirrored_store(out):
    def store(rows, upper, lower, value):
        value = value.astype(BF16)
        out[rows, upper] = value
        if lower.start < B:
            out[lower, rows] = value[:, TILE:].T

    return store


def plus_diagonal(value, scale):
    row = lax.broadcasted_iota(jnp.int32, value.shape, 0)
    col = lax.broadcasted_iota(jnp.int32, value.shape, 1)
    return jnp.where(row == col, 1.25, 0.0) - scale * value


def factor_store(factor_out, matrix_out):
    def store(rows, upper, lower, value):
        factor = plus_diagonal(value, 0.25).astype(BF16)
        factor_out[rows, upper] = factor
        if lower.start < B:
            factor_out[lower, rows] = factor[:, TILE:].T
        if matrix_out is not None:
            matrix = value.astype(BF16)
            matrix_out[rows, upper] = matrix
            if lower.start < B:
                matrix_out[lower, rows] = matrix[:, TILE:].T

    return store


def roots_kernel(
    whole, gram, clip_in, old, accum_in, statistic_new, root_a, factor, matrix_out, accum_new,
    new, matrix, square, fourth, norm, accum_sem, tile_sem,
):
    core = lax.axis_index("c")
    put_accum = pltpu.make_async_copy(accum_in, accum_new, accum_sem)
    put_accum.start()
    known = (NT - 1) * TILE

    clip = clip_in[0:1, 0:1]
    weight = 0.1 / B * clip * clip

    def update(products):
        frob = jnp.zeros((8, 128), F32)
        for (rows, upper, lower), product in zip(panels(), products):
            product = product * weight
            value = 0.9 * old[rows, upper] + product
            new[rows, upper] = value
            frob += to_tile(value * value)
            if lower.start < B:
                value = 0.9 * old[lower, rows] + product[:, TILE:].T
                new[lower, rows] = value
                frob += to_tile(value * value)
        norm[...] = frob

    @pl.when(core == 0)
    def _():
        last = dot(whole[...], whole[known:, :], 1, 1)
        parts = [
            jnp.concatenate([gram[rows, upper.start : known], last[rows]], axis=1)
            for rows, upper, _ in list(panels())[: NT - 1]
        ]
        update(parts + [last[known:]])

    @pl.when(core == 1)
    def _():
        update(
            dot(whole[known:, rows], whole[known:, upper], 0, 0) + gram[rows, upper]
            for rows, upper, _ in panels()
        )

    frob = norm[...]
    put_tiles = started(
        [
            pltpu.make_async_copy(new.at[kept], statistic_new.at[theirs], tile_sem.at[i])
            for i, kept, theirs in statistic_tiles()
        ]
    )
    total = jnp.sum(frob, axis=(0, 1), keepdims=True)
    scale = 2.5 / jnp.sqrt(total + 1e-06)
    start = jnp.sqrt(jnp.sqrt(scale)).astype(BF16).astype(F32)

    @pl.loop(0, B // ROWS)
    def _(i):
        rows = pl.ds(pl.multiple_of(i * ROWS, ROWS), ROWS)
        value = scale * new[rows, :]
        matrix[rows, :] = value.astype(BF16)
        row = lax.broadcasted_iota(jnp.int32, value.shape, 0) + i * ROWS
        col = lax.broadcasted_iota(jnp.int32, value.shape, 1)
        step = (jnp.where(row == col, 1.25, 0.0) - 0.25 * value).astype(BF16)
        factor[rows, :] = step
        root_a[rows, :] = (start * step.astype(F32)).astype(BF16)

    symmetric_product(factor, factor, mirrored_store(square))
    symmetric_product(square, square, mirrored_store(fourth))
    symmetric_product(fourth, matrix, factor_store(factor, matrix_out))
    put_accum.wait()
    for copy in put_tiles:
        copy.wait()


def roots(whole, gram, clip, statistic, accum):
    return pl.pallas_call(
        roots_kernel,
        name="roots",
        out_shape=(
            jax.ShapeDtypeStruct((B, B), F32),
            jax.ShapeDtypeStruct((B, B), BF16),
            jax.ShapeDtypeStruct((B, B), BF16),
            jax.ShapeDtypeStruct((B, B), BF16),
            jax.ShapeDtypeStruct((CHIPS, ROWS, B), F32),
        ),
        in_specs=[VMEM, VMEM, VMEM, VMEM, VMEM],
        out_specs=(HBM, VMEM, VMEM, VMEM, HBM),
        scratch_shapes=[pltpu.VMEM((B, B), F32)]
        + [pltpu.VMEM((B, B), BF16)] * 3
        + [pltpu.VMEM((8, 128), F32)]
        + [pltpu.SemaphoreType.DMA, pltpu.SemaphoreType.DMA((NT * NT,))],
        compiler_params=pltpu.CompilerParams(vmem_limit_bytes=32 << 20),
    )(whole, gram, clip, statistic, accum)


def apply_kernel(
    root_a, factor_a, matrix, whole, graft, back, ratio_out,
    root, factor, square, fourth, both, applied, product, tile1, slots1, tile2, slots2,
    left_sem, right_sem, bulk_sem, plane_sem, column_sem,
):
    place = Place()
    place.greet()

    def swap_left(j):
        chips = pl.ds(4 * j, 4)
        return remote(
            both.at[0, chips, 1], both.at[0, chips, 1],
            left_sem.at[0, j], left_sem.at[1, j], place.partner,
        )

    def swap_right(j):
        part = (1, pl.ds(4 * j, 4), slice(None), slice(None), pl.ds(j * TILE, B - j * TILE))
        return remote(
            both.at[part], both.at[part], right_sem.at[0, j], right_sem.at[1, j], place.partner
        )

    def give_back(j, i):
        return remote(
            product.at[j, place.slot_to(PLANE[i])], back.at[j, place.chip],
            bulk_sem.at[0, j, i], bulk_sem.at[1, j, i], place.plane(PLANE[i]),
        )

    symmetric_product(root_a, factor_a, mirrored_store(root))
    symmetric_product(factor_a, factor_a, mirrored_store(square))
    symmetric_product(square, square, mirrored_store(fourth))
    symmetric_product(fourth, matrix, factor_store(factor, None))
    place.met()
    for j, (rows, upper, lower) in enumerate(panels()):
        value = dot(root[rows, :], factor[:, upper], 1, 0).astype(BF16)
        both[place.c, 4 * j : 4 * j + 4, :, :, upper] = value.reshape(4, 2, ROWS, -1)
        if lower.start < B:
            mirror = value[:, TILE:].T
            both[place.c, 4 * j + 4 : CHIPS, :, :, rows] = mirror.reshape(-1, 2, ROWS, TILE)

        if j % 2:

            @pl.when(place.c == 0)
            def _(j=j):
                swap_left(j - 1).start()
                swap_left(j).start()

            @pl.when(place.c == 1)
            def _(j=j):
                swap_right(j - 1).start()
                swap_right(j).start()

    for half in range(2):

        @pl.when(place.c == 1)
        def _(half=half):
            for j in (2 * half, 2 * half + 1):
                swap_left(j).wait_recv()

        left_rows = both[0, 8 * half : 8 * half + 8, place.c].reshape(TILE, B)
        applied[half * TILE : (half + 1) * TILE] = dot(left_rows, whole[...], 1, 0).astype(BF16)
    squares = jnp.zeros((8, 128), F32)
    for j, (rows, upper, _) in enumerate(panels()):

        if j == 0:

            @pl.when(place.c == 0)
            def _():
                for i in range(NT):
                    swap_right(i).wait_recv()

        right_rows = both[1, 4 * j : 4 * j + 4, :, :, upper].reshape(TILE, -1)
        value = dot(applied[:, upper], right_rows, 1, 1)
        if j:
            value += dot(applied[:, : j * TILE], both[1, : 4 * j, :, :, rows].reshape(-1, TILE), 1, 0)
        squares += to_tile(value * value)
        product[j] = value.astype(BF16).reshape(CHIPS, ROWS, TILE)
        if j == NT - 1:
            tile1[0:8] = squares
            tile1[8:16] = graft[...]
            plane = started(plane_sends(place, tile1, slots1, plane_sem))
        for panel in {0: [0], NT - 1: range(1, NT)}.get(j, []):
            for i in RETURN:
                give_back(panel, i).start()
        back[j, place.chip] = product[j, place.z]

    tile2[...] = gathered(plane, tile1, slots1, place.chip)
    column = started(column_sends(place, tile2, slots2, column_sem))
    total = gathered(column, tile2, slots2, place.column)
    update_total = jnp.sum(total[0:8], axis=(0, 1), keepdims=True)
    graft_total = jnp.sum(total[8:16], axis=(0, 1), keepdims=True)
    ratio_out[...] = jnp.broadcast_to(jnp.sqrt(graft_total / (update_total + 1e-06)), (8, 128))

    @pl.when(place.c == 0)
    def _():
        for j in range(NT):
            swap_left(j).wait_send()

    @pl.when(place.c == 1)
    def _():
        for j in range(NT):
            swap_right(j).wait_send()

    for j in range(NT):
        for i in range(len(PLANE)):
            give_back(j, i).wait()


def apply(root, factor, matrix, whole, graft):
    return pl.pallas_call(
        apply_kernel,
        name="apply",
        out_shape=(
            jax.ShapeDtypeStruct((NT, CHIPS, ROWS, TILE), BF16),
            jax.ShapeDtypeStruct((8, 128), F32),
        ),
        in_specs=[VMEM, VMEM, VMEM, VMEM, VMEM],
        out_specs=(VMEM, VMEM),
        scratch_shapes=[pltpu.VMEM((B, B), BF16)] * 4
        + [
            pltpu.VMEM((2, CHIPS, 2, ROWS, B), BF16),
            pltpu.VMEM((B // 2, B), BF16),
            pltpu.VMEM((NT, CHIPS, ROWS, TILE), BF16),
            pltpu.VMEM((16, 128), F32),
            pltpu.VMEM((CHIPS, 16, 128), F32),
            pltpu.VMEM((16, 128), F32),
            pltpu.VMEM((8, 16, 128), F32),
            pltpu.SemaphoreType.DMA((2, NT)),
            pltpu.SemaphoreType.DMA((2, NT)),
            pltpu.SemaphoreType.DMA((2, NT, 15)),
            pltpu.SemaphoreType.DMA((2, 15)),
            pltpu.SemaphoreType.DMA((2, 7)),
        ],
        compiler_params=pltpu.CompilerParams(
            collective_id=1, has_side_effects=True, vmem_limit_bytes=32 << 20
        ),
    )(root, factor, matrix, whole, graft)


def scale_kernel(back, ratio, update, wide, sems):
    factor = ratio[0:1, 0:1]
    puts = []
    for group in range(4):
        for chip in range(4 * group, 4 * group + 4):
            for j in range(NT):
                wide[chip, :, j * TILE : (j + 1) * TILE] = factor * back[j, chip].astype(F32)
        chips = pl.ds(4 * group, 4)
        puts += started([pltpu.make_async_copy(wide.at[chips], update.at[chips], sems.at[group])])
    for put in puts:
        put.wait()


def scale(back, ratio):
    return pl.pallas_call(
        scale_kernel,
        name="scale",
        out_shape=jax.ShapeDtypeStruct((CHIPS, ROWS, B), F32),
        in_specs=[VMEM, VMEM],
        out_specs=HBM,
        scratch_shapes=[pltpu.VMEM((CHIPS, ROWS, B), F32), pltpu.SemaphoreType.DMA((4,))],
        compiler_params=pltpu.CompilerParams(vmem_limit_bytes=16 << 20),
    )(back, ratio)


def on_device(gradients, statistics, accumulator):
    in_hbm = functools.partial(
        pltpu.with_memory_space_constraint, memory_space=pltpu.MemorySpace.HBM
    )
    grads = gradients.reshape(CHIPS, ROWS, B)
    whole, clip, accum, graft, statistic, gram = gather(
        in_hbm(grads), in_hbm(accumulator.reshape(CHIPS, ROWS, B)), in_hbm(statistics.reshape(B, B))
    )
    whole = whole.reshape(B, B)
    statistic_new, root, factor, matrix, accum_new = roots(whole, gram, clip, statistic, accum)
    update = scale(*apply(root, factor, matrix, whole, graft))
    return (
        update.reshape(gradients.shape),
        statistic_new.reshape(statistics.shape),
        accum_new.reshape(accumulator.shape),
    )


def solution(mesh):
    finer = Mesh(mesh.devices.reshape(4, 4, 2, mesh.shape["mp"]), ("y", "z", "c", "mp"))
    dp = ("y", "z", "c")
    specs = (P(None, "mp", dp, None), P("mp", dp, None, None), P(None, "mp", dp, None))
    return jax.shard_map(on_device, mesh=finer, in_specs=specs, out_specs=specs, check_vma=False)
```

```python
import functools

import jax
import jax.numpy as jnp
from jax import lax
from jax.experimental import pallas as pl
from jax.experimental.pallas import tpu as pltpu
from jax.sharding import Mesh
from jax.sharding import PartitionSpec as P

F32 = jnp.float32
BF16 = jnp.bfloat16
MESH = pl.DeviceIdType.MESH
VMEM = pl.BlockSpec(memory_space=pltpu.VMEM)
HBM = pl.BlockSpec(memory_space=pltpu.MemorySpace.HBM)

B = 1024
TILE = 256
NT = B // TILE
ROWS = 32
CHIPS = 16
ENTRIES = 4 * 16 * 1024 * 1024


def ring_distance(offset):
    return sum(min(step, 4 - step) for step in offset)


PLANE = sorted(
    [(dy, dz) for dy in range(4) for dz in range(4) if (dy, dz) != (0, 0)],
    key=lambda offset: (offset[0] == 2, ring_distance(offset)),
)
COLUMN = [(dx, dc) for dx in range(4) for dc in range(2) if (dx, dc) != (0, 0)]

ORDER = (0, 1, 3, 2)
POSITION = [ORDER.index(step) for step in range(4)]
SEND = sorted(range(len(PLANE)), key=lambda i: ring_distance(PLANE[i]))
RETURN = sorted(range(len(PLANE)), key=lambda i: -ring_distance(PLANE[i]))
EARLY = sum(offset[0] != 2 for offset in PLANE)


class Place:
    def __init__(self):
        self.y, self.z, self.c, self.x = (lax.axis_index(a) for a in ("y", "z", "c", "mp"))
        self.chip = self.y * 4 + self.z
        self.column = self.x * 2 + self.c
        self.partner = {"c": 1 - self.c}

    def plane(self, offset):
        return {"y": lax.rem(self.y + offset[0], 4), "z": lax.rem(self.z + offset[1], 4)}

    def plane_chip(self, offset):
        return lax.rem(self.y + offset[0], 4) * 4 + lax.rem(self.z + offset[1], 4)

    def slot_to(self, offset):
        return POSITION[offset[0]] * 4 + lax.rem(self.z + offset[1], 4)

    def slot_from(self, offset):
        return POSITION[(4 - offset[0]) % 4] * 4 + lax.rem(self.z + 4 - offset[1], 4)

    def landing(self, offset):
        return POSITION[(4 - offset[0]) % 4] * 4 + self.z

    def in_column(self, offset):
        return {"mp": lax.rem(self.x + offset[0], 4), "c": lax.rem(self.c + offset[1], 2)}

    def greet(self):
        barrier = pltpu.get_barrier_semaphore()
        for offset in PLANE:
            pl.semaphore_signal(barrier, 1, device_id=self.plane(offset), device_id_type=MESH)
        for offset in COLUMN:
            pl.semaphore_signal(barrier, 1, device_id=self.in_column(offset), device_id_type=MESH)

    def met(self):
        pl.semaphore_wait(pltpu.get_barrier_semaphore(), len(PLANE) + len(COLUMN))


def statistic_tiles():
    y, c = lax.axis_index("y"), lax.axis_index("c")
    starts = [((1 - c) * lax.rem(y + ORDER[p], 4) + c * p) * TILE for p in range(NT)]
    windows = [pl.ds(pl.multiple_of(start, TILE), TILE) for start in starts]
    for p in range(NT):
        for q in range(NT):
            kept = (slice(p * TILE, (p + 1) * TILE), slice(q * TILE, (q + 1) * TILE))
            yield p * NT + q, kept, (windows[p], windows[q])


def remote(src, dst, send, recv, device):
    return pltpu.make_async_remote_copy(
        src_ref=src, dst_ref=dst, send_sem=send, recv_sem=recv, device_id=device, device_id_type=MESH
    )


def started(copies):
    for copy in copies:
        copy.start()
    return copies


def to_tile(value):
    value = value.reshape(-1, 8, value.shape[-1]).sum(0)
    return sum(value[:, k * 128 : (k + 1) * 128] for k in range(value.shape[1] // 128))


def plane_sends(place, tile, slots, sems):
    return [
        remote(tile, slots.at[place.chip], sems.at[0, i], sems.at[1, i], place.plane(offset))
        for i, offset in enumerate(PLANE)
    ]


def column_sends(place, tile, slots, sems):
    return [
        remote(tile, slots.at[place.column], sems.at[0, i], sems.at[1, i], place.in_column(offset))
        for i, offset in enumerate(COLUMN)
    ]


def gathered(copies, tile, slots, own):
    slots[own] = tile[...]
    for copy in copies:
        copy.wait()
    return functools.reduce(jnp.add, [slots[k] for k in range(slots.shape[0])])


def gather_kernel(
    grads, accum, statistic, whole, clip_out, accum_new, graft_out, statistic_out, gram,
    own, accum_in, tile1, slots1, tile2, slots2,
    load_sem, tile_sem, bulk_sem, pass_sem, plane_sem, column_sem,
):
    place = Place()
    load_grads = pltpu.make_async_copy(grads, own, load_sem.at[0])
    load_accum = pltpu.make_async_copy(accum, accum_in, load_sem.at[1])
    load_grads.start()
    place.greet()
    load_grads.wait()
    squares = jnp.zeros((8, B), F32)
    for block in range(CHIPS):
        wide = own[block].astype(F32)
        squares += (wide * wide).reshape(-1, 8, B).sum(0)
    tile1[...] = to_tile(squares)
    load_accum.start()
    load_tiles = started(
        [
            pltpu.make_async_copy(statistic.at[theirs], statistic_out.at[kept], tile_sem.at[i])
            for i, kept, theirs in statistic_tiles()
        ]
    )
    place.met()
    plane = started(plane_sends(place, tile1, slots1, plane_sem))
    bulk = [
        remote(
            own.at[place.plane_chip(offset)], whole.at[place.landing(offset), place.c],
            bulk_sem.at[0, i], bulk_sem.at[1, i], place.plane(offset),
        )
        for i, offset in enumerate(PLANE)
    ]
    started([bulk[i] for i in SEND])

    def pass_on(i):
        bulk[i].wait_recv()
        slot = place.slot_from(PLANE[i])
        return started(
            [
                remote(
                    whole.at[slot, place.c], whole.at[slot, place.c],
                    pass_sem.at[0, i], pass_sem.at[1, i], place.partner,
                )
            ]
        )

    passed = started(
        [
            remote(
                own.at[place.chip], whole.at[place.z, place.c],
                pass_sem.at[0, 15], pass_sem.at[1, 15], place.partner,
            )
        ]
    )
    whole[place.z, place.c] = own[place.chip]
    tile2[...] = gathered(plane, tile1, slots1, place.chip)
    column = started(column_sends(place, tile2, slots2, column_sem))
    load_accum.wait()
    total = jnp.sum(gathered(column, tile2, slots2, place.column), axis=(0, 1), keepdims=True)
    clip = jnp.minimum(1.0, jnp.sqrt(ENTRIES / (total + 1e-06)))
    clip_out[...] = jnp.broadcast_to(clip, (8, 128))
    graft = jnp.zeros((8, B), F32)
    for i in range(CHIPS):
        if i < EARLY:
            passed += pass_on(i)
        scaled = clip * own[i].astype(F32)
        square = scaled * scaled
        accumulated = accum_in[i] + square
        accum_new[i] = accumulated
        graft += (square / accumulated).reshape(-1, 8, B).sum(0)
    graft_out[...] = to_tile(graft)
    for i in range(EARLY, len(PLANE)):
        passed += pass_on(i)
    for copy in passed[: EARLY + 1]:
        copy.wait_recv()
    early_gram(place.c, whole, gram)
    for copy in load_tiles:
        copy.wait()
    for copy in bulk:
        copy.wait_send()
    for copy in passed[: EARLY + 1]:
        copy.wait_send()
    for copy in passed[EARLY + 1 :]:
        copy.wait()


def early_gram(core, whole, gram):
    known = (NT - 1) * TILE

    @pl.when(core == 0)
    def _():
        rows = whole[:12].reshape(known, B)
        for j in range(NT - 1):
            part = rows[j * TILE :]
            gram[j * TILE : (j + 1) * TILE, j * TILE : known] = dot(part[:TILE], part, 1, 1)

    @pl.when(core == 1)
    def _():
        for rows, upper, _ in panels():
            left = whole[:12, :, :, rows].reshape(known, TILE)
            gram[rows, upper] = dot(left, whole[:12, :, :, upper].reshape(known, -1), 0, 0)


def gather(grads, accum, statistic):
    return pl.pallas_call(
        gather_kernel,
        name="gather",
        out_shape=(
            jax.ShapeDtypeStruct((CHIPS, 2, ROWS, B), BF16),
            jax.ShapeDtypeStruct((8, 128), F32),
            jax.ShapeDtypeStruct((CHIPS, ROWS, B), F32),
            jax.ShapeDtypeStruct((8, 128), F32),
            jax.ShapeDtypeStruct((B, B), F32),
            jax.ShapeDtypeStruct((B, B), F32),
        ),
        in_specs=[HBM, HBM, HBM],
        out_specs=(VMEM, VMEM, VMEM, VMEM, VMEM, VMEM),
        scratch_shapes=[
            pltpu.VMEM((CHIPS, ROWS, B), BF16),
            pltpu.VMEM((CHIPS, ROWS, B), F32),
            pltpu.VMEM((8, 128), F32),
            pltpu.VMEM((CHIPS, 8, 128), F32),
            pltpu.VMEM((8, 128), F32),
            pltpu.VMEM((8, 8, 128), F32),
            pltpu.SemaphoreType.DMA((2,)),
            pltpu.SemaphoreType.DMA((NT * NT,)),
            pltpu.SemaphoreType.DMA((2, 15)),
            pltpu.SemaphoreType.DMA((2, 16)),
            pltpu.SemaphoreType.DMA((2, 15)),
            pltpu.SemaphoreType.DMA((2, 7)),
        ],
        compiler_params=pltpu.CompilerParams(collective_id=0, has_side_effects=True, vmem_limit_bytes=24 << 20),
    )(grads, accum, statistic)


def dot(left, right, contract_left, contract_right):
    return lax.dot_general(
        left, right, (((contract_left,), (contract_right,)), ((), ())), preferred_element_type=F32
    )


def panels():
    for j in range(NT):
        yield slice(j * TILE, (j + 1) * TILE), slice(j * TILE, B), slice((j + 1) * TILE, B)


def symmetric_product(left, right, store):
    for rows, upper, lower in panels():
        value = dot(left[rows, :], right[:, upper], 1, 0)
        store(rows, upper, lower, value)


def mirrored_store(out):
    def store(rows, upper, lower, value):
        value = value.astype(BF16)
        out[rows, upper] = value
        if lower.start < B:
            out[lower, rows] = value[:, TILE:].T

    return store


def plus_diagonal(value, scale):
    square = value[:, :TILE]
    row = lax.broadcasted_iota(jnp.int32, square.shape, 0)
    col = lax.broadcasted_iota(jnp.int32, square.shape, 1)
    square = jnp.where(row == col, 1.25 - scale * square, -scale * square)
    if value.shape[1] == TILE:
        return square
    return jnp.concatenate([square, -scale * value[:, TILE:]], axis=1)


def factor_store(factor_out, matrix_out):
    def store(rows, upper, lower, value):
        factor = plus_diagonal(value, 0.25).astype(BF16)
        factor_out[rows, upper] = factor
        if lower.start < B:
            factor_out[lower, rows] = factor[:, TILE:].T
        if matrix_out is not None:
            matrix = value.astype(BF16)
            matrix_out[rows, upper] = matrix
            if lower.start < B:
                matrix_out[lower, rows] = matrix[:, TILE:].T

    return store


def roots_kernel(
    whole, gram, clip_in, old, accum_in, statistic_new, root_a, factor, matrix_out, accum_new,
    new, matrix, square, fourth, norm, accum_sem, tile_sem,
):
    core = lax.axis_index("c")
    put_accum = pltpu.make_async_copy(accum_in, accum_new, accum_sem)
    put_accum.start()
    known = (NT - 1) * TILE

    clip = clip_in[0:1, 0:1]
    weight = 0.1 / B * clip * clip

    def update(products):
        frob = jnp.zeros((8, 128), F32)
        for (rows, upper, lower), product in zip(panels(), products):
            product = product * weight
            value = 0.9 * old[rows, upper] + product
            new[rows, upper] = value
            frob += to_tile(value * value)
            if lower.start < B:
                value = 0.9 * old[lower, rows] + product[:, TILE:].T
                new[lower, rows] = value
                frob += to_tile(value * value)
        norm[...] = frob

    @pl.when(core == 0)
    def _():
        last = dot(whole[...], whole[known:, :], 1, 1)
        parts = [
            jnp.concatenate([gram[rows, upper.start : known], last[rows]], axis=1)
            for rows, upper, _ in list(panels())[: NT - 1]
        ]
        update(parts + [last[known:]])

    @pl.when(core == 1)
    def _():
        update(
            dot(whole[known:, rows], whole[known:, upper], 0, 0) + gram[rows, upper]
            for rows, upper, _ in panels()
        )

    frob = norm[...]
    put_tiles = started(
        [
            pltpu.make_async_copy(new.at[kept], statistic_new.at[theirs], tile_sem.at[i])
            for i, kept, theirs in statistic_tiles()
        ]
    )
    total = jnp.sum(frob, axis=(0, 1), keepdims=True)
    scale = 2.5 / jnp.sqrt(total + 1e-06)
    start = jnp.sqrt(jnp.sqrt(scale)).astype(BF16)

    def first_step(rows, cols, diagonal):
        value = scale * new[rows, cols]
        matrix[rows, cols] = value.astype(BF16)
        step = -0.25 * value
        if diagonal is not None:
            row = lax.broadcasted_iota(jnp.int32, value.shape, 0) + diagonal
            col = lax.broadcasted_iota(jnp.int32, value.shape, 1)
            step = jnp.where(row == col, 1.25 + step, step)
        step = step.astype(BF16)
        factor[rows, cols] = step
        root_a[rows, cols] = start * step

    for block in range(NT):
        inside = slice(block * TILE, (block + 1) * TILE)

        @pl.loop(0, TILE // ROWS)
        def _(i, block=block, inside=inside):
            rows = pl.ds(pl.multiple_of(block * TILE + i * ROWS, ROWS), ROWS)
            first_step(rows, inside, i * ROWS)
            if block:
                first_step(rows, slice(0, inside.start), None)
            if block < NT - 1:
                first_step(rows, slice(inside.stop, B), None)

    symmetric_product(factor, factor, mirrored_store(square))
    symmetric_product(square, square, mirrored_store(fourth))
    symmetric_product(fourth, matrix, factor_store(factor, matrix_out))
    put_accum.wait()
    for copy in put_tiles:
        copy.wait()


def roots(whole, gram, clip, statistic, accum):
    return pl.pallas_call(
        roots_kernel,
        name="roots",
        out_shape=(
            jax.ShapeDtypeStruct((B, B), F32),
            jax.ShapeDtypeStruct((B, B), BF16),
            jax.ShapeDtypeStruct((B, B), BF16),
            jax.ShapeDtypeStruct((B, B), BF16),
            jax.ShapeDtypeStruct((CHIPS, ROWS, B), F32),
        ),
        in_specs=[VMEM, VMEM, VMEM, VMEM, VMEM],
        out_specs=(HBM, VMEM, VMEM, VMEM, HBM),
        scratch_shapes=[pltpu.VMEM((B, B), F32)]
        + [pltpu.VMEM((B, B), BF16)] * 3
        + [pltpu.VMEM((8, 128), F32)]
        + [pltpu.SemaphoreType.DMA, pltpu.SemaphoreType.DMA((NT * NT,))],
        compiler_params=pltpu.CompilerParams(vmem_limit_bytes=32 << 20),
    )(whole, gram, clip, statistic, accum)


def apply_kernel(
    root_a, factor_a, matrix, whole, graft, back, ratio_out,
    root, factor, square, fourth, both, applied, product, tile1, slots1, tile2, slots2,
    left_sem, right_sem, bulk_sem, plane_sem, column_sem,
):
    place = Place()
    place.greet()

    def swap_left(j):
        chips = pl.ds(4 * j, 4)
        return remote(
            both.at[0, chips, 1], both.at[0, chips, 1],
            left_sem.at[0, j], left_sem.at[1, j], place.partner,
        )

    def swap_right(j):
        part = (1, pl.ds(4 * j, 4), slice(None), slice(None), pl.ds(j * TILE, B - j * TILE))
        return remote(
            both.at[part], both.at[part], right_sem.at[0, j], right_sem.at[1, j], place.partner
        )

    def give_back(j, i):
        return remote(
            product.at[j, place.slot_to(PLANE[i])], back.at[j, place.chip],
            bulk_sem.at[0, j, i], bulk_sem.at[1, j, i], place.plane(PLANE[i]),
        )

    symmetric_product(root_a, factor_a, mirrored_store(root))
    symmetric_product(factor_a, factor_a, mirrored_store(square))
    symmetric_product(square, square, mirrored_store(fourth))
    symmetric_product(fourth, matrix, factor_store(factor, None))
    place.met()
    for j, (rows, upper, lower) in enumerate(panels()):
        value = dot(root[rows, :], factor[:, upper], 1, 0).astype(BF16)
        both[place.c, 4 * j : 4 * j + 4, :, :, upper] = value.reshape(4, 2, ROWS, -1)
        if lower.start < B:
            mirror = value[:, TILE:].T
            both[place.c, 4 * j + 4 : CHIPS, :, :, rows] = mirror.reshape(-1, 2, ROWS, TILE)

        if j % 2:

            @pl.when(place.c == 0)
            def _(j=j):
                swap_left(j - 1).start()
                swap_left(j).start()

            @pl.when(place.c == 1)
            def _(j=j):
                swap_right(j - 1).start()
                swap_right(j).start()

    for half in range(2):

        @pl.when(place.c == 1)
        def _(half=half):
            for j in (2 * half, 2 * half + 1):
                swap_left(j).wait_recv()

        left_rows = both[0, 8 * half : 8 * half + 8, place.c].reshape(TILE, B)
        applied[half * TILE : (half + 1) * TILE] = dot(left_rows, whole[...], 1, 0).astype(BF16)
    squares = jnp.zeros((8, 128), F32)
    for j, (rows, upper, _) in enumerate(panels()):

        if j % 2 == 0:

            @pl.when(place.c == 0)
            def _(j=j):
                swap_right(j).wait_recv()
                swap_right(j + 1).wait_recv()

        right_rows = both[1, 4 * j : 4 * j + 4, :, :, upper].reshape(TILE, -1)
        value = dot(applied[:, upper], right_rows, 1, 1)
        if j:
            value += dot(applied[:, : j * TILE], both[1, : 4 * j, :, :, rows].reshape(-1, TILE), 1, 0)
        squares += to_tile(value * value)
        product[j] = value.astype(BF16).reshape(CHIPS, ROWS, TILE)
        if j == NT - 1:
            tile1[0:8] = squares
            tile1[8:16] = graft[...]
            plane = started(plane_sends(place, tile1, slots1, plane_sem))
        for panel in {0: [0], NT - 1: range(1, NT)}.get(j, []):
            for i in RETURN:
                give_back(panel, i).start()
        back[j, place.chip] = product[j, place.z]

    tile2[...] = gathered(plane, tile1, slots1, place.chip)
    column = started(column_sends(place, tile2, slots2, column_sem))
    total = gathered(column, tile2, slots2, place.column)
    update_total = jnp.sum(total[0:8], axis=(0, 1), keepdims=True)
    graft_total = jnp.sum(total[8:16], axis=(0, 1), keepdims=True)
    ratio_out[...] = jnp.broadcast_to(jnp.sqrt(graft_total / (update_total + 1e-06)), (8, 128))

    @pl.when(place.c == 0)
    def _():
        for j in range(NT):
            swap_left(j).wait_send()

    @pl.when(place.c == 1)
    def _():
        for j in range(NT):
            swap_right(j).wait_send()

    for j in range(NT):
        for i in range(len(PLANE)):
            give_back(j, i).wait()


def apply(root, factor, matrix, whole, graft):
    return pl.pallas_call(
        apply_kernel,
        name="apply",
        out_shape=(
            jax.ShapeDtypeStruct((NT, CHIPS, ROWS, TILE), BF16),
            jax.ShapeDtypeStruct((8, 128), F32),
        ),
        in_specs=[VMEM, VMEM, VMEM, VMEM, VMEM],
        out_specs=(VMEM, VMEM),
        scratch_shapes=[pltpu.VMEM((B, B), BF16)] * 4
        + [
            pltpu.VMEM((2, CHIPS, 2, ROWS, B), BF16),
            pltpu.VMEM((B // 2, B), BF16),
            pltpu.VMEM((NT, CHIPS, ROWS, TILE), BF16),
            pltpu.VMEM((16, 128), F32),
            pltpu.VMEM((CHIPS, 16, 128), F32),
            pltpu.VMEM((16, 128), F32),
            pltpu.VMEM((8, 16, 128), F32),
            pltpu.SemaphoreType.DMA((2, NT)),
            pltpu.SemaphoreType.DMA((2, NT)),
            pltpu.SemaphoreType.DMA((2, NT, 15)),
            pltpu.SemaphoreType.DMA((2, 15)),
            pltpu.SemaphoreType.DMA((2, 7)),
        ],
        compiler_params=pltpu.CompilerParams(
            collective_id=1, has_side_effects=True, vmem_limit_bytes=32 << 20
        ),
    )(root, factor, matrix, whole, graft)


def scale_kernel(back, ratio, update, wide, sems):
    factor = ratio[0:1, 0:1]
    puts = []
    for group in range(4):
        for chip in range(4 * group, 4 * group + 4):
            for j in range(NT):
                wide[chip, :, j * TILE : (j + 1) * TILE] = factor * back[j, chip].astype(F32)
        chips = pl.ds(4 * group, 4)
        puts += started([pltpu.make_async_copy(wide.at[chips], update.at[chips], sems.at[group])])
    for put in puts:
        put.wait()


def scale(back, ratio):
    return pl.pallas_call(
        scale_kernel,
        name="scale",
        out_shape=jax.ShapeDtypeStruct((CHIPS, ROWS, B), F32),
        in_specs=[VMEM, VMEM],
        out_specs=HBM,
        scratch_shapes=[pltpu.VMEM((CHIPS, ROWS, B), F32), pltpu.SemaphoreType.DMA((4,))],
        compiler_params=pltpu.CompilerParams(vmem_limit_bytes=16 << 20),
    )(back, ratio)


def on_device(gradients, statistics, accumulator):
    in_hbm = functools.partial(
        pltpu.with_memory_space_constraint, memory_space=pltpu.MemorySpace.HBM
    )
    grads = gradients.reshape(CHIPS, ROWS, B)
    whole, clip, accum, graft, statistic, gram = gather(
        in_hbm(grads), in_hbm(accumulator.reshape(CHIPS, ROWS, B)), in_hbm(statistics.reshape(B, B))
    )
    whole = whole.reshape(B, B)
    statistic_new, root, factor, matrix, accum_new = roots(whole, gram, clip, statistic, accum)
    update = scale(*apply(root, factor, matrix, whole, graft))
    return (
        update.reshape(gradients.shape),
        statistic_new.reshape(statistics.shape),
        accum_new.reshape(accumulator.shape),
    )


def solution(mesh):
    finer = Mesh(mesh.devices.reshape(4, 4, 2, mesh.shape["mp"]), ("y", "z", "c", "mp"))
    dp = ("y", "z", "c")
    specs = (P(None, "mp", dp, None), P("mp", dp, None, None), P(None, "mp", dp, None))
    return jax.shard_map(on_device, mesh=finer, in_specs=specs, out_specs=specs, check_vma=False)
```
